8 devices in a mesh: dp: 2 (over y, z), sp: 4 (over x, core).
Axes of the slice: x: 2, y: 2, z: 1, core: 2. Of those that a mesh axis runs over, the one named last changes fastest.
Arguments:
- x: bfloat16 [4096, 6144], P(('dp', 'sp')), parts along dimension 0
- gain: bfloat16 [6144], replicated
- wq: bfloat16 [6144, 6144], replicated
- wk: bfloat16 [6144, 1024], replicated
- wv: bfloat16 [6144, 1024], replicated
- wo: bfloat16 [6144, 6144], replicated
Outputs:
- output: bfloat16 [4096, 6144], P(('dp', 'sp')), parts along dimension 0
There are 2 independent parts. The reference program is written for one: setup_inputs(seed, part) draws one part's arguments, and reference() takes and returns one part's arrays. A program takes and returns all parts, laid end to end along the dimension named above; an argument that names none is the same for every part.
All inputs are finite; a program needn't handle non-finite values.
Results may differ from the reference program's by a relative error of at most 0.012.
Values are sent between devices in bfloat16 or wider.
A program may use at most 2 GiB of HBM per device.

```python
import jax
import jax.numpy as jnp
from jax import lax

ROWS = 2048
D = 6144
HEADS = 48
KV_HEADS = 8
HEAD = 128
THETA = 10000


def setup_inputs(seed: int = 0, part: int = 0) -> dict:
    kx, kn, kq, kk, kv, ko = jax.random.split(jax.random.key(seed), 6)

    def weights(key, rows, columns):
        return jax.random.normal(key, (rows, columns), jnp.float32) * rows**-0.5

    drawn = {
        "x": jax.random.normal(jax.random.fold_in(kx, part), (ROWS, D), jnp.float32),
        "gain": 1 + 0.1 * jax.random.normal(kn, (D,), jnp.float32),
        "wq": 2 * weights(kq, D, HEADS * HEAD),
        "wk": 2 * weights(kk, D, KV_HEADS * HEAD),
        "wv": 4 * weights(kv, D, KV_HEADS * HEAD),
        "wo": weights(ko, HEADS * HEAD, D),
    }
    return {k: v.astype(jnp.bfloat16) for k, v in drawn.items()}


def normed(x, gain):
    wide = x.astype(jnp.float32)
    scale = lax.rsqrt(jnp.mean(wide * wide, -1, keepdims=True) + 1e-6)
    return (wide * scale * gain.astype(jnp.float32)).astype(jnp.bfloat16)


def turned(t, place, theta):
    half = t.shape[-1] // 2
    angle = place.astype(jnp.float32)[:, None] * theta ** (-jnp.arange(half, dtype=jnp.float32) / half)
    cos, sin = jnp.cos(angle)[:, None], jnp.sin(angle)[:, None]
    a, b = t[..., :half].astype(jnp.float32), t[..., half:].astype(jnp.float32)
    return jnp.concatenate([a * cos - b * sin, b * cos + a * sin], -1).astype(jnp.bfloat16)


def matmul(a, w):
    return jnp.dot(a, w, preferred_element_type=jnp.float32).astype(jnp.bfloat16)


def einsum(form, a, b):
    return jnp.einsum(form, a.astype(jnp.float32), b.astype(jnp.float32))


def attention(q, k, v):
    scores = einsum("tgsd,ugd->gstu", q, k) * q.shape[-1] ** -0.5
    token = jnp.arange(q.shape[0])
    scores = jnp.where(token[:, None] >= token, scores, -jnp.inf)
    weights = jax.nn.softmax(scores, -1).astype(jnp.bfloat16)
    return einsum("gstu,ugd->tgsd", weights, v).astype(jnp.bfloat16)


def reference(x, gain, wq, wk, wv, wo):
    a, place = normed(x, gain), jnp.arange(ROWS)
    q = turned(matmul(a, wq).reshape(ROWS, HEADS, HEAD), place, THETA).reshape(ROWS, KV_HEADS, -1, HEAD)
    k = turned(matmul(a, wk).reshape(ROWS, KV_HEADS, HEAD), place, THETA)
    v = matmul(a, wv).reshape(ROWS, KV_HEADS, HEAD)
    seen = attention(q, k, v).reshape(ROWS, HEADS * HEAD)
    return (x.astype(jnp.float32) + jnp.dot(seen, wo, preferred_element_type=jnp.float32)).astype(jnp.bfloat16)
```

```python
import functools

import jax
import jax.numpy as jnp
from jax import lax
from jax.experimental import pallas as pl
from jax.experimental.pallas import tpu as pltpu
from jax.sharding import PartitionSpec as P

HEAD = 128
THETA = 10000
NEG = -1e30
HIDDEN = 2 * NEG
E2 = HEAD**-0.5 * 1.4426950408889634
OWN = 512
D = 6144
HALF = 3072
KVH = 512
BF, F32 = jnp.bfloat16, jnp.float32


def dot(a, b, ca=1, cb=0):
    return lax.dot_general(a, b, (((ca,), (cb,)), ((), ())), preferred_element_type=F32)


def turn(t, cos, sin):
    return (t * cos + pltpu.roll(t, HEAD // 2, 1) * sin).astype(BF)


def tables(first):
    half = HEAD // 2
    place = (first + jnp.arange(OWN)).astype(F32)[:, None]
    angle = place * THETA ** (-jnp.arange(half, dtype=F32) / half)
    cos, sin = jnp.cos(angle), jnp.sin(angle)
    return jnp.concatenate([cos, cos], 1), jnp.concatenate([-sin, sin], 1)


def _kv(sc, x_ref, g_ref, wk_ref, wv_ref, cos_ref, sin_ref, a_ref, k_ref, v_ref):
    j = pl.program_id(0)

    @pl.when(j == 0)
    def _():
        for r in range(0, OWN, 64):
            wide = x_ref[r : r + 64, :].astype(F32)
            scale = lax.rsqrt(jnp.mean(wide * wide, -1, keepdims=True) + 1e-6)
            a_ref[r : r + 64, :] = (wide * scale * g_ref[...].astype(F32)).astype(BF)

    @pl.when(j < 2)
    def _():
        k = dot(a_ref[...], wk_ref[...]).astype(BF).astype(F32)
        for h in range(2):
            k_ref[:, h * HEAD : (h + 1) * HEAD] = turn(k[:, h * HEAD : (h + 1) * HEAD], cos_ref[...], sin_ref[...])

    @pl.when(j >= 2)
    def _():
        v_ref[...] = dot(a_ref[...], wv_ref[...]).T.astype(BF)


def keys_values(x, gain, wk, wv, cos, sin, core):
    whole = lambda s: pl.BlockSpec(s, lambda j, sc: (0, 0), pipeline_mode=pl.Buffered(1))
    return pl.pallas_call(
        _kv,
        grid_spec=pltpu.PrefetchScalarGridSpec(
            num_scalar_prefetch=1,
            grid=(4,),
            in_specs=[
                whole((OWN, D)),
                whole((1, D)),
                pl.BlockSpec((D, 256), lambda j, sc: (0, sc[0] * 2 + jnp.minimum(j, 1))),
                pl.BlockSpec((D, 256), lambda j, sc: (0, sc[0] * 2 + jnp.maximum(j - 2, 0))),
                whole((OWN, HEAD)),
                whole((OWN, HEAD)),
            ],
            out_specs=[
                pl.BlockSpec((OWN, D), lambda j, sc: (0, 0)),
                pl.BlockSpec((OWN, 256), lambda j, sc: (0, jnp.minimum(j, 1))),
                pl.BlockSpec((256, OWN), lambda j, sc: (jnp.maximum(j - 2, 0), 0)),
            ],
        ),
        out_shape=[
            jax.ShapeDtypeStruct((OWN, D), BF),
            jax.ShapeDtypeStruct((OWN, KVH), BF),
            jax.ShapeDtypeStruct((KVH, OWN), BF),
        ],
        compiler_params=pltpu.CompilerParams(dimension_semantics=("arbitrary",), vmem_limit_bytes=48 * 2**20),
        cost_estimate=pl.CostEstimate(flops=2 * OWN * D * 2 * KVH, bytes_accessed=4 * D * KVH + 4 * OWN * D, transcendentals=0),
        name="keys_values",
    )(core, x, gain, wk, wv, cos, sin)


def _q(sc, a0_ref, a1_ref, w_ref, c0_ref, s0_ref, c1_ref, s1_ref, q0_ref, q1_ref):
    for a_ref, c_ref, s_ref, q_ref in ((a1_ref, c1_ref, s1_ref, q1_ref), (a0_ref, c0_ref, s0_ref, q0_ref)):
        q = dot(a_ref[...], w_ref[...]).astype(BF).astype(F32)
        for h in range(q.shape[1] // HEAD):
            at = slice(h * HEAD, (h + 1) * HEAD)
            q_ref[:, at] = turn(q[:, at], c_ref[...], s_ref[...])


def queries(a0, a1, wq, t0, t1, core, bn=256):
    whole = lambda s: pl.BlockSpec(s, lambda j, sc: (0, 0), pipeline_mode=pl.Buffered(1))
    out = pl.BlockSpec((OWN, bn), lambda j, sc: (0, j))
    return pl.pallas_call(
        _q,
        grid_spec=pltpu.PrefetchScalarGridSpec(
            num_scalar_prefetch=1,
            grid=(HALF // bn,),
            in_specs=[whole((OWN, D)), whole((OWN, D)), pl.BlockSpec((D, bn), lambda j, sc: (0, sc[0] * (HALF // bn) + j))]
            + [whole((OWN, HEAD))] * 4,
            out_specs=[out, out],
        ),
        out_shape=[jax.ShapeDtypeStruct((OWN, HALF), BF)] * 2,
        compiler_params=pltpu.CompilerParams(dimension_semantics=("arbitrary",), vmem_limit_bytes=40 * 2**20),
        cost_estimate=pl.CostEstimate(flops=4 * OWN * D * HALF, bytes_accessed=2 * D * HALF + 4 * OWN * D, transcendentals=0),
        name="queries",
    )(core, a0, a1, wq, *t0, *t1)


def _attend(sc, q_ref, k_ref, v_ref, ko_ref, vo_ref, r0_ref, u0_ref, r1_ref, u1_ref, o_ref, top_s, mix_s, *, lead, lag):
    group, ones = 6, 16
    top_s[...] = jnp.full(top_s.shape, NEG, F32)
    mix_s[...] = jnp.zeros(mix_s.shape, F32)

    def run(kref, vref, hidden):
        scores, weights = [None] * group, [None] * group

        def score(h):
            scores[h] = dot(kref[...], q_ref[:, h * HEAD : (h + 1) * HEAD], 1, 1)

        def weigh(h):
            s, at = scores[h], slice(h * OWN, (h + 1) * OWN)
            if hidden:
                s = jnp.where(lax.broadcasted_iota(jnp.int32, s.shape, 0) <= lax.broadcasted_iota(jnp.int32, s.shape, 1), s, HIDDEN)
            old = top_s[0:1, at]
            top = jnp.maximum(old, s.max(axis=0, keepdims=True))
            top_s[0:1, at] = top
            weights[h] = jnp.exp2((s - top) * E2).astype(BF), jnp.exp2((old - top) * E2)

        def mix(h):
            (p, keep), at = weights[h], slice(h * OWN, (h + 1) * OWN)
            values = jnp.concatenate([vref[...], jnp.ones((ones, OWN), BF)], 0)
            mix_s[:, at] = mix_s[:, at] * keep + dot(values, p)

        for t in range(group + lead + lag):
            if t < group:
                score(t)
            if 0 <= t - lead < group:
                weigh(t - lead)
            if 0 <= t - lead - lag < group:
                mix(t - lead - lag)

    @pl.when(sc[0] == 1)
    def _():
        run(r0_ref, u0_ref, False)
        run(r1_ref, u1_ref, False)

    @pl.when(sc[1] == 1)
    def _():
        run(ko_ref, vo_ref, False)

    run(k_ref, v_ref, True)
    for h in range(group):
        at = slice(h * OWN, (h + 1) * OWN)
        o_ref[:, h * HEAD : (h + 1) * HEAD] = (mix_s[:HEAD, at] * (1 / mix_s[HEAD : HEAD + 1, at])).T.astype(BF)


def attend(q, k, v, ko, vo, r0, u0, r1, u1, chip, later, lead=2, lag=1):
    keys = pl.BlockSpec((OWN, HEAD), lambda g, s: (0, g))
    values = pl.BlockSpec((HEAD, OWN), lambda g, s: (g, 0))
    return pl.pallas_call(
        functools.partial(_attend, lead=lead, lag=lag),
        grid_spec=pltpu.PrefetchScalarGridSpec(
            num_scalar_prefetch=1,
            grid=(4,),
            in_specs=[pl.BlockSpec((OWN, 768), lambda g, s: (0, g))] + [keys, values] * 4,
            out_specs=pl.BlockSpec((OWN, 768), lambda g, s: (0, g)),
            scratch_shapes=[pltpu.VMEM((8, 6 * OWN), F32), pltpu.VMEM((HEAD + 16, 6 * OWN), F32)],
        ),
        out_shape=jax.ShapeDtypeStruct((OWN, HALF), BF),
        compiler_params=pltpu.CompilerParams(dimension_semantics=("arbitrary",), vmem_limit_bytes=40 * 2**20),
        cost_estimate=pl.CostEstimate(flops=24 * OWN * 1536 * 512, bytes_accessed=16 * 2**20, transcendentals=24 * OWN * 1536),
        name="attend",
    )(jnp.stack([chip, later]).astype(jnp.int32), q, k, v, ko, vo, r0, u0, r1, u1)


def _out(sc, x_ref, o0_ref, o1_ref, w0_ref, w1_ref, y_ref):
    y = dot(o0_ref[...], w0_ref[...]) + dot(o1_ref[...], w1_ref[...])
    y_ref[...] = (x_ref[...].astype(F32) + y).astype(BF)


def output(x, o0, o1, wo, core, bn=512):
    whole = lambda s: pl.BlockSpec(s, lambda j, sc: (0, 0), pipeline_mode=pl.Buffered(1))
    cols = pl.BlockSpec((OWN, bn), lambda j, sc: (0, j))
    return pl.pallas_call(
        _out,
        grid_spec=pltpu.PrefetchScalarGridSpec(
            num_scalar_prefetch=1,
            grid=(D // bn,),
            in_specs=[
                cols,
                whole((OWN, HALF)),
                whole((OWN, HALF)),
                pl.BlockSpec((HALF, bn), lambda j, sc: (sc[0], j)),
                pl.BlockSpec((HALF, bn), lambda j, sc: (1 - sc[0], j)),
            ],
            out_specs=cols,
        ),
        out_shape=jax.ShapeDtypeStruct((OWN, D), BF),
        compiler_params=pltpu.CompilerParams(dimension_semantics=("arbitrary",), vmem_limit_bytes=48 * 2**20),
        cost_estimate=pl.CostEstimate(flops=2 * OWN * D * D, bytes_accessed=2 * D * D + 6 * OWN * D, transcendentals=0),
        name="output",
    )(core, x, o0, o1, wo, wo)


SWAP = [(0, 1), (1, 0), (2, 3), (3, 2)]
OVER = [(0, 2), (1, 3)]


def solution(mesh):
    def step(x, gain, wq, wk, wv, wo):
        sp = lax.axis_index("sp")
        core, chip = sp % 2, sp // 2
        pick = jnp.reshape(core, (1,)).astype(jnp.int32)
        swap = lambda t: lax.ppermute(t, "sp", SWAP)
        over = lambda t: lax.ppermute(t, "sp", OVER)
        x1 = swap(x)
        t0, t1 = tables(sp * OWN), tables((sp + 1 - 2 * core) * OWN)
        gain = gain[None]
        a0, k0, v0 = keys_values(x, gain, wk, wv, *t0, pick)
        r0, u0 = over(k0), over(v0)
        a1, k1, v1 = keys_values(x1, gain, wk, wv, *t1, pick)
        r1, u1 = over(k1), over(v1)
        q0, q1 = queries(a0, a1, wq, t0, t1, pick)
        o1 = attend(q1, k1, v1, k0, v0, r0, u0, r1, u1, chip, 1 - core)
        mine = swap(o1)
        o0 = attend(q0, k0, v0, k1, v1, r0, u0, r1, u1, chip, core)
        return output(x, o0, mine, wo, pick)

    tokens, whole = P(("dp", "sp"), None), P(None, None)
    return jax.shard_map(
        step,
        mesh=mesh,
        in_specs=(tokens, P(None), whole, whole, whole, whole),
        out_specs=tokens,
        check_vma=False,
    )
```

```python
import functools

import jax
import jax.numpy as jnp
from jax import lax
from jax.experimental import pallas as pl
from jax.experimental.pallas import tpu as pltpu
from jax.sharding import PartitionSpec as P

HEAD = 128
THETA = 10000
NEG = -1e30
HIDDEN = 2 * NEG
E2 = HEAD**-0.5 * 1.4426950408889634
OWN = 512
D = 6144
HALF = 3072
KVH = 512
BF, F32 = jnp.bfloat16, jnp.float32


def dot(a, b, ca=1, cb=0):
    return lax.dot_general(a, b, (((ca,), (cb,)), ((), ())), preferred_element_type=F32)


def turn(t, cos, sin):
    return (t * cos + pltpu.roll(t, HEAD // 2, 1) * sin).astype(BF)


def tables(first):
    half = HEAD // 2
    place = (first + jnp.arange(OWN)).astype(F32)[:, None]
    angle = place * THETA ** (-jnp.arange(half, dtype=F32) / half)
    cos, sin = jnp.cos(angle), jnp.sin(angle)
    return jnp.concatenate([cos, cos], 1), jnp.concatenate([-sin, sin], 1)


CHUNK = 128
TILE = 512
TILES = HALF // TILE
MESH = pl.DeviceIdType.MESH


def _qkv(x_hbm, g_ref, cos_ref, sin_ref, wq, wk, wv, q_hbm, k_hbm, v_hbm, xs, w, kv, qs, xsem, xsend, xrecv, wsem, kvsem, ksend, krecv, qsem):
    sp = lax.axis_index("sp")
    core, chip = lax.rem(sp, 2), lax.div(sp, 2)
    mate, peer = sp + 1 - 2 * core, lax.rem(sp + 2, 4)

    def rows(i):
        return pl.ds(i * CHUNK, CHUNK)

    def weight(n):
        if n < 2:
            src = (wk, wv)[n].at[:, pl.ds(pl.multiple_of(core * KVH, KVH), KVH)]
        else:
            src = wq.at[:, pl.ds(pl.multiple_of(core * HALF + (n - 2) * TILE, TILE), TILE)]
        return pltpu.make_async_copy(src, w.at[n % 4], wsem.at[n % 4])

    mine = [pltpu.make_async_copy(x_hbm.at[rows(i)], xs.at[0, rows(i)], xsem.at[i]) for i in range(OWN // CHUNK)]
    for c in mine:
        c.start()
    for n in range(4):
        weight(n).start()
    barrier = pltpu.get_barrier_semaphore()
    for other in (mate, peer):
        pl.semaphore_signal(barrier, inc=1, device_id={"sp": other}, device_id_type=MESH)
    pl.semaphore_wait(barrier, 2)
    swaps = [
        pltpu.make_async_remote_copy(
            src_ref=x_hbm.at[rows(i)], dst_ref=xs.at[1, rows(i)], send_sem=xsend.at[i], recv_sem=xrecv.at[i],
            device_id={"sp": mate}, device_id_type=MESH)
        for i in range(OWN // CHUNK)
    ]
    for c in swaps:
        c.start()

    def norm(s, at, n):
        wide = xs[s, pl.ds(at, n), :].astype(F32)
        scale = lax.rsqrt(jnp.mean(wide * wide, -1, keepdims=True) + 1e-6)
        xs[s, pl.ds(at, n), :] = (wide * scale * g_ref[...]).astype(BF)

    for i, c in enumerate(mine):
        c.wait()
        lax.fori_loop(0, CHUNK // 32, lambda r, _: norm(0, pl.multiple_of(i * CHUNK + r * 32, 32), 32), None)
    weight(0).wait()
    weight(1).wait()

    def turned_to(dst, t, s, at, n):
        for h in range(TILE // HEAD):
            one = slice(h * HEAD, (h + 1) * HEAD)
            dst[:, one] = turn(t[:, one], cos_ref[s, pl.ds(at, n), :], sin_ref[s, pl.ds(at, n), :])

    def leave(s, p):
        block, n = lax.rem(core + s, 2), 2 * s + p
        out = (k_hbm, v_hbm)[p]
        return (
            pltpu.make_async_copy(kv.at[n], out.at[2 + block], kvsem.at[n]),
            pltpu.make_async_remote_copy(
                src_ref=kv.at[n], dst_ref=out.at[block], send_sem=ksend.at[n], recv_sem=krecv.at[n],
                device_id={"sp": peer}, device_id_type=MESH),
        )

    def send(s, p):
        here, there = leave(s, p)
        here.start()

        @pl.when(chip == 0)
        def _():
            there.start()

    def q_out(i):
        s, tile = lax.rem(i, 2), lax.div(i, 2)
        return pltpu.make_async_copy(
            qs.at[s], q_hbm.at[lax.rem(core + s, 2), :, pl.ds(pl.multiple_of(tile * TILE, TILE), TILE)], qsem.at[s])

    def keys_values(s, _):
        k = dot(xs[s], w[0]).astype(BF).astype(F32)
        turned_to(kv.at[2 * s], k, s, 0, OWN)
        send(s, 0)
        kv[2 * s + 1] = dot(xs[s], w[1]).T.astype(BF)
        send(s, 1)

        @pl.when(s == 0)
        def _():
            weight(2).wait()
            for i, c in enumerate(swaps):
                c.wait_recv()
                q = dot(xs[0, rows(i), :], w[2]).astype(BF).astype(F32)
                for r in range(0, CHUNK, 32):
                    norm(1, i * CHUNK + r, 32)
                turned_to(qs.at[0, rows(i)], q, 0, i * CHUNK, CHUNK)
            q_out(0).start()

    lax.fori_loop(0, 2, keys_values, None)
    weight(4).start()
    weight(5).start()

    def item(i, _):
        s, tile = lax.rem(i, 2), lax.div(i, 2)
        slot = lax.rem(tile + 2, 4)

        @pl.when((s == 0))
        def _():
            pltpu.make_async_copy(wq.at[:, pl.ds(0, TILE)], w.at[slot], wsem.at[slot]).wait()

        @pl.when(i >= 2)
        def _():
            q_out(i - 2).wait()

        q = dot(xs[s], w[slot]).astype(BF).astype(F32)
        turned_to(qs.at[s], q, s, 0, OWN)
        q_out(i).start()
        for t in range(2):
            @pl.when(i == 2 * t + 1)
            def _():
                weight(6 + t).start()

    lax.fori_loop(1, 2 * TILES, item, None)
    for i in (2 * TILES - 2, 2 * TILES - 1):
        q_out(i).wait()
    for c in swaps:
        c.wait_send()
    for s in range(2):
        for p in range(2):
            here, there = leave(s, p)
            here.wait()

            @pl.when(chip == 0)
            def _():
                there.wait_send()

            @pl.when(chip == 1)
            def _():
                there.wait_recv()


def project(x, gain, cos, sin, wq, wk, wv):
    vmem, hbm = pl.BlockSpec(memory_space=pltpu.VMEM), pl.BlockSpec(memory_space=pl.ANY)
    dma = pltpu.SemaphoreType.DMA
    return pl.pallas_call(
        _qkv,
        in_specs=[hbm, vmem, vmem, vmem, hbm, hbm, hbm],
        out_specs=[hbm] * 3,
        out_shape=[
            jax.ShapeDtypeStruct((2, OWN, HALF), BF),
            jax.ShapeDtypeStruct((4, OWN, KVH), BF),
            jax.ShapeDtypeStruct((4, KVH, OWN), BF),
        ],
        scratch_shapes=[
            pltpu.VMEM((2, OWN, D), BF), pltpu.VMEM((4, D, TILE), BF), pltpu.VMEM((4, OWN, KVH), BF), pltpu.VMEM((2, OWN, TILE), BF),
            dma((4,)), dma((4,)), dma((4,)), dma((4,)), dma((4,)), dma((4,)), dma((4,)), dma((2,)),
        ],
        compiler_params=pltpu.CompilerParams(collective_id=0, has_side_effects=True, vmem_limit_bytes=60 * 2**20),
        cost_estimate=pl.CostEstimate(flops=4 * OWN * D * (HALF + 2 * KVH), bytes_accessed=2 * D * (HALF + 2 * KVH) + 8 * OWN * D, transcendentals=0),
        name="project",
    )(x, gain, cos, sin, wq, wk, wv)


def _attend(sc, q_ref, k_ref, v_ref, ko_ref, vo_ref, r0_ref, u0_ref, r1_ref, u1_ref, o_ref, top_s, mix_s, *, lead, lag):
    group, ones = 6, 16
    top_s[...] = jnp.full(top_s.shape, NEG, F32)
    mix_s[...] = jnp.zeros(mix_s.shape, F32)

    def run(kref, vref, hidden):
        scores, weights = [None] * group, [None] * group

        def score(h):
            scores[h] = dot(kref[...], q_ref[:, h * HEAD : (h + 1) * HEAD], 1, 1)

        def weigh(h):
            s, at = scores[h], slice(h * OWN, (h + 1) * OWN)
            if hidden:
                s = jnp.where(lax.broadcasted_iota(jnp.int32, s.shape, 0) <= lax.broadcasted_iota(jnp.int32, s.shape, 1), s, HIDDEN)
            old = top_s[0:1, at]
            top = jnp.maximum(old, s.max(axis=0, keepdims=True))
            top_s[0:1, at] = top
            weights[h] = jnp.exp2((s - top) * E2).astype(BF), jnp.exp2((old - top) * E2)

        def mix(h):
            (p, keep), at = weights[h], slice(h * OWN, (h + 1) * OWN)
            values = jnp.concatenate([vref[...], jnp.ones((ones, OWN), BF)], 0)
            mix_s[:, at] = mix_s[:, at] * keep + dot(values, p)

        for t in range(group + lead + lag):
            if t < group:
                score(t)
            if 0 <= t - lead < group:
                weigh(t - lead)
            if 0 <= t - lead - lag < group:
                mix(t - lead - lag)

    @pl.when(sc[0] == 1)
    def _():
        run(r0_ref, u0_ref, False)
        run(r1_ref, u1_ref, False)

    @pl.when(sc[1] == 1)
    def _():
        run(ko_ref, vo_ref, False)

    run(k_ref, v_ref, True)
    for h in range(group):
        at = slice(h * OWN, (h + 1) * OWN)
        o_ref[:, h * HEAD : (h + 1) * HEAD] = (mix_s[:HEAD, at] * (1 / mix_s[HEAD : HEAD + 1, at])).T.astype(BF)


def attend(q, k, v, chip, block, lead=2, lag=1):
    keys = lambda f: pl.BlockSpec((None, OWN, HEAD), lambda g, s: (f(s), 0, g))
    values = lambda f: pl.BlockSpec((None, HEAD, OWN), lambda g, s: (f(s), g, 0))
    places = (lambda s: 2 + s[1], lambda s: 3 - s[1], lambda s: 0, lambda s: 1)
    return pl.pallas_call(
        functools.partial(_attend, lead=lead, lag=lag),
        grid_spec=pltpu.PrefetchScalarGridSpec(
            num_scalar_prefetch=1,
            grid=(4,),
            in_specs=[pl.BlockSpec((None, OWN, 768), lambda g, s: (s[1], 0, g))] + [f(p) for p in places for f in (keys, values)],
            out_specs=pl.BlockSpec((OWN, 768), lambda g, s: (0, g)),
            scratch_shapes=[pltpu.VMEM((8, 6 * OWN), F32), pltpu.VMEM((HEAD + 16, 6 * OWN), F32)],
        ),
        out_shape=jax.ShapeDtypeStruct((OWN, HALF), BF),
        compiler_params=pltpu.CompilerParams(dimension_semantics=("arbitrary",), vmem_limit_bytes=40 * 2**20),
        cost_estimate=pl.CostEstimate(flops=24 * OWN * 1536 * 512, bytes_accessed=16 * 2**20, transcendentals=24 * OWN * 1536),
        name="attend",
    )(jnp.stack([chip, block]).astype(jnp.int32), q, *[k, v] * 4)


def _out(sc, x_ref, o0_ref, o1_ref, w0_ref, w1_ref, y_ref):
    y = dot(o0_ref[...], w0_ref[...]) + dot(o1_ref[...], w1_ref[...])
    y_ref[...] = (x_ref[...].astype(F32) + y).astype(BF)


def output(x, o0, o1, wo, core, bn=512):
    whole = lambda s: pl.BlockSpec(s, lambda j, sc: (0, 0), pipeline_mode=pl.Buffered(1))
    cols = pl.BlockSpec((OWN, bn), lambda j, sc: (0, j))
    return pl.pallas_call(
        _out,
        grid_spec=pltpu.PrefetchScalarGridSpec(
            num_scalar_prefetch=1,
            grid=(D // bn,),
            in_specs=[
                cols,
                whole((OWN, HALF)),
                whole((OWN, HALF)),
                pl.BlockSpec((HALF, bn), lambda j, sc: (sc[0], j)),
                pl.BlockSpec((HALF, bn), lambda j, sc: (1 - sc[0], j)),
            ],
            out_specs=cols,
        ),
        out_shape=jax.ShapeDtypeStruct((OWN, D), BF),
        compiler_params=pltpu.CompilerParams(dimension_semantics=("arbitrary",), vmem_limit_bytes=48 * 2**20),
        cost_estimate=pl.CostEstimate(flops=2 * OWN * D * D, bytes_accessed=2 * D * D + 6 * OWN * D, transcendentals=0),
        name="output",
    )(core, x, o0, o1, wo, wo)


SWAP = [(0, 1), (1, 0), (2, 3), (3, 2)]


def solution(mesh):
    def step(x, gain, wq, wk, wv, wo):
        sp = lax.axis_index("sp")
        core, chip = sp % 2, sp // 2
        pick = jnp.reshape(core, (1,)).astype(jnp.int32)
        tabs = [tables(sp * OWN), tables((sp + 1 - 2 * core) * OWN)]
        cos, sin = (jnp.stack([t[i] for t in tabs]) for i in range(2))
        q, k, v = project(x, gain.astype(F32)[None], cos, sin, wq, wk, wv)
        o1 = attend(q, k, v, chip, 1 - core)
        mine = lax.ppermute(o1, "sp", SWAP)
        o0 = attend(q, k, v, chip, core)
        return output(x, o0, mine, wo, pick)

    tokens, whole = P(("dp", "sp"), None), P(None, None)
    return jax.shard_map(
        step,
        mesh=mesh,
        in_specs=(tokens, P(None), whole, whole, whole, whole),
        out_specs=tokens,
        check_vma=False,
    )
```

```python
import functools

import jax
import jax.numpy as jnp
from jax import lax
from jax.experimental import pallas as pl
from jax.experimental.pallas import tpu as pltpu
from jax.sharding import PartitionSpec as P

HEAD = 128
THETA = 10000
NEG = -1e30
HIDDEN = 2 * NEG
E2 = HEAD**-0.5 * 1.4426950408889634
OWN = 512
D = 6144
HALF = 3072
KVH = 512
BF, F32 = jnp.bfloat16, jnp.float32


def dot(a, b, ca=1, cb=0):
    return lax.dot_general(a, b, (((ca,), (cb,)), ((), ())), preferred_element_type=F32)


def turn(t, cos, sin):
    return (t * cos + pltpu.roll(t, HEAD // 2, 1) * sin).astype(BF)


def tables(first, second):
    half = HEAD // 2
    row = jnp.arange(2 * OWN)
    place = jnp.where(row < OWN, first + row, second + row - OWN).astype(F32)
    angle = place[:, None] * THETA ** (-jnp.arange(half, dtype=F32) / half)
    return jnp.cos(angle), jnp.sin(angle)


CHUNK = 128
TILE = 512
TILES = HALF // TILE
MESH = pl.DeviceIdType.MESH


def _project(x_hbm, g_ref, c_ref, s_ref, wq, wk, wv, q_hbm, k_hbm, v_hbm, xs, w, kv, qs, gain, cos, sin, xsem, xsend, xrecv, wsem, kvsem, ksend, krecv, qsem):
    sp = lax.axis_index("sp")
    core, chip = lax.rem(sp, 2), lax.div(sp, 2)
    mate, peer = sp + 1 - 2 * core, lax.rem(sp + 2, 4)

    def rows(i):
        return pl.ds(i * CHUNK, CHUNK)

    def weight(n):
        if isinstance(n, int) and n < 2:
            src = (wk, wv)[n].at[:, pl.ds(pl.multiple_of(core * KVH, KVH), KVH)]
        else:
            src = wq.at[:, pl.ds(pl.multiple_of(core * HALF + (n - 2) * TILE, TILE), TILE)]
        slot = lax.rem(n, 4)
        return pltpu.make_async_copy(src, w.at[slot], wsem.at[slot])

    mine = [pltpu.make_async_copy(x_hbm.at[rows(i)], xs.at[rows(i)], xsem.at[i]) for i in range(OWN // CHUNK)]
    for c in mine:
        c.start()
    for n in range(4):
        weight(n).start()
    barrier = pltpu.get_barrier_semaphore()
    for other in (mate, peer):
        pl.semaphore_signal(barrier, inc=1, device_id={"sp": other}, device_id_type=MESH)
    pl.semaphore_wait(barrier, 2)
    swaps = [
        pltpu.make_async_remote_copy(
            src_ref=x_hbm.at[rows(i)], dst_ref=xs.at[pl.ds(OWN + i * CHUNK, CHUNK)], send_sem=xsend.at[i], recv_sem=xrecv.at[i],
            device_id={"sp": mate}, device_id_type=MESH)
        for i in range(OWN // CHUNK)
    ]
    for c in swaps:
        c.start()
    gain[...] = g_ref[...].astype(F32)
    cos[...] = jnp.concatenate([c_ref[...], c_ref[...]], 1)
    sin[...] = jnp.concatenate([-s_ref[...], s_ref[...]], 1)

    def norm(at, n):
        wide = xs[pl.ds(at, n), :].astype(F32)
        scale = lax.rsqrt(jnp.mean(wide * wide, -1, keepdims=True) + 1e-6)
        xs[pl.ds(at, n), :] = (wide * scale * gain[...]).astype(BF)

    for i, c in enumerate(mine):
        c.wait()
        lax.fori_loop(0, CHUNK // 32, lambda r, _: norm(pl.multiple_of(i * CHUNK + r * 32, 32), 32), None)
    weight(0).wait()
    weight(1).wait()

    def turned_to(dst, t, at):
        n = t.shape[0]
        t = t.astype(BF).astype(F32)
        for h in range(TILE // HEAD):
            one = slice(h * HEAD, (h + 1) * HEAD)
            dst[:, one] = turn(t[:, one], cos[pl.ds(at, n), :], sin[pl.ds(at, n), :])

    def leave(s, p):
        block, n = lax.rem(core + s, 2), 2 * s + p
        out = (k_hbm, v_hbm)[p]
        return (
            pltpu.make_async_copy(kv.at[n], out.at[2 + block], kvsem.at[n]),
            pltpu.make_async_remote_copy(
                src_ref=kv.at[n], dst_ref=out.at[block], send_sem=ksend.at[n], recv_sem=krecv.at[n],
                device_id={"sp": peer}, device_id_type=MESH),
        )

    def send(s, p):
        here, there = leave(s, p)
        here.start()

        @pl.when(chip == 0)
        def _():
            there.start()

    def q_out(tile, s):
        cols = pl.ds(pl.multiple_of(tile * TILE, TILE), TILE)
        part = lax.rem(tile, 2)
        return pltpu.make_async_copy(qs.at[part, pl.ds(s * OWN, OWN)], q_hbm.at[lax.rem(core + s, 2), :, cols], qsem.at[part, s])

    def keys_values(s, _):
        at = pl.multiple_of(s * OWN, OWN)
        turned_to(kv.at[2 * s], dot(xs[pl.ds(at, OWN), :], w[0]), at)
        send(s, 0)
        kv[2 * s + 1] = dot(xs[pl.ds(at, OWN), :], w[1]).T.astype(BF)
        send(s, 1)

        @pl.when(s == 0)
        def _():
            weight(2).wait()
            for i, c in enumerate(swaps):
                c.wait_recv()
                q = dot(xs[rows(i), :], w[2])
                for r in range(0, CHUNK, 32):
                    norm(OWN + i * CHUNK + r, 32)
                turned_to(qs.at[0, rows(i)], q, i * CHUNK)

    lax.fori_loop(0, 2, keys_values, None)
    weight(4).start()
    weight(5).start()
    weight(3).wait()
    turned_to(qs.at[0, pl.ds(OWN, OWN)], dot(xs[pl.ds(OWN, OWN), :], w[2]), OWN)
    for s in range(2):
        q_out(0, s).start()
    weight(6).start()

    def tile(t, _):
        @pl.when(t < TILES - 1)
        def _():
            weight(t + 3).wait()

        @pl.when(t >= 2)
        def _():
            for s in range(2):
                q_out(t - 2, s).wait()

        turned_to(qs.at[lax.rem(t, 2)], dot(xs[...], w[lax.rem(t + 2, 4)]), 0)
        for s in range(2):
            q_out(t, s).start()

        @pl.when(t == 1)
        def _():
            weight(7).start()

    lax.fori_loop(1, TILES, tile, None)
    for t in (TILES - 2, TILES - 1):
        for s in range(2):
            q_out(t, s).wait()
    for c in swaps:
        c.wait_send()
    for s in range(2):
        for p in range(2):
            here, there = leave(s, p)
            here.wait()

            @pl.when(chip == 0)
            def _():
                there.wait_send()

            @pl.when(chip == 1)
            def _():
                there.wait_recv()


def project(x, gain, cos, sin, wq, wk, wv):
    vmem, hbm = pl.BlockSpec(memory_space=pltpu.VMEM), pl.BlockSpec(memory_space=pl.ANY)
    dma = pltpu.SemaphoreType.DMA
    return pl.pallas_call(
        _project,
        in_specs=[hbm, vmem, vmem, vmem, hbm, hbm, hbm],
        out_specs=[hbm] * 3,
        out_shape=[
            jax.ShapeDtypeStruct((2, OWN, HALF), BF),
            jax.ShapeDtypeStruct((4, OWN, KVH), BF),
            jax.ShapeDtypeStruct((4, KVH, OWN), BF),
        ],
        scratch_shapes=[
            pltpu.VMEM((2 * OWN, D), BF), pltpu.VMEM((4, D, TILE), BF), pltpu.VMEM((4, OWN, KVH), BF), pltpu.VMEM((2, 2 * OWN, TILE), BF),
            pltpu.VMEM((1, D), F32), pltpu.VMEM((2 * OWN, HEAD), F32), pltpu.VMEM((2 * OWN, HEAD), F32),
            dma((4,)), dma((4,)), dma((4,)), dma((4,)), dma((4,)), dma((4,)), dma((4,)), dma((2, 2)),
        ],
        compiler_params=pltpu.CompilerParams(collective_id=0, has_side_effects=True, vmem_limit_bytes=62 * 2**20),
        cost_estimate=pl.CostEstimate(flops=4 * OWN * D * (HALF + 2 * KVH), bytes_accessed=2 * D * (HALF + 2 * KVH) + 8 * OWN * D, transcendentals=0),
        name="project",
    )(x, gain, cos, sin, wq, wk, wv)


GROUP = 6
STRIP = 256


def _attend(q_hbm, k_hbm, v_hbm, o_hbm, q, k, v, o, qsem, ksem, osem, osend, orecv):
    sp = lax.axis_index("sp")
    core, chip = lax.rem(sp, 2), lax.div(sp, 2)
    mate = sp + 1 - 2 * core

    def load(g):
        slot = lax.rem(g, 2)
        wide, one = pl.ds(pl.multiple_of(g * GROUP * HEAD, HEAD), GROUP * HEAD), pl.ds(pl.multiple_of(g * HEAD, HEAD), HEAD)
        return (
            [pltpu.make_async_copy(q_hbm.at[b, :, wide], q.at[slot, pl.ds(b * OWN, OWN)], qsem.at[slot, b]) for b in range(2)]
            + [pltpu.make_async_copy(k_hbm.at[b, :, one], k.at[slot, pl.ds(b * OWN, OWN)], ksem.at[slot, 0, b]) for b in range(4)]
            + [pltpu.make_async_copy(v_hbm.at[b, one, :], v.at[slot, :, pl.ds(b * OWN, OWN)], ksem.at[slot, 1, b]) for b in range(4)]
        )

    def leave(g):
        slot = lax.rem(g, 2)
        cols = pl.ds(pl.multiple_of(core * HALF + g * GROUP * HEAD, HEAD), GROUP * HEAD)
        own, others = (pl.ds(pl.multiple_of(c * OWN, OWN), OWN) for c in (core, 1 - core))
        return (
            pltpu.make_async_copy(o.at[slot, own], o_hbm.at[:, cols], osem.at[slot]),
            pltpu.make_async_remote_copy(
                src_ref=o.at[slot, others], dst_ref=o_hbm.at[:, cols], send_sem=osend.at[g], recv_sem=orecv.at[g],
                device_id={"sp": mate}, device_id_type=MESH),
        )

    for c in load(0):
        c.start()
    barrier = pltpu.get_barrier_semaphore()
    pl.semaphore_signal(barrier, inc=1, device_id={"sp": mate}, device_id_type=MESH)
    pl.semaphore_wait(barrier, 1)

    def attention(slot, first):
        items = [(h, i) for h in range(GROUP) for i in range(2 * OWN // STRIP)]
        scores, weights = {}, {}

        def end(i):
            return 2 * OWN + (i + 1) * STRIP

        def score(t):
            h, i = items[t]
            queries = q[slot, i * STRIP : (i + 1) * STRIP, h * HEAD : (h + 1) * HEAD]
            scores[t] = [dot(k[slot, a : min(a + 512, end(i)), :], queries, 1, 1) for a in range(first, end(i), 512)]

        def weigh(t):
            s = scores.pop(t)
            cut = s[-1].shape[0] - STRIP
            ok = lax.broadcasted_iota(jnp.int32, (STRIP, STRIP), 0) <= lax.broadcasted_iota(jnp.int32, (STRIP, STRIP), 1)
            s = s[:-1] + ([s[-1][:cut]] if cut else []) + [jnp.where(ok, s[-1][cut:], HIDDEN)]
            top = functools.reduce(jnp.maximum, [x.max(axis=0, keepdims=True) for x in s])
            weights[t] = [jnp.exp2((x - top) * E2).astype(BF) for x in s]

        def mix(t):
            h, i = items[t]
            values = jnp.concatenate([v[slot, :, first : end(i)], jnp.ones((16, end(i) - first), BF)], 0)
            m = dot(values, jnp.concatenate(weights.pop(t), 0))
            o[slot, i * STRIP : (i + 1) * STRIP, h * HEAD : (h + 1) * HEAD] = (m[:HEAD] * (1 / m[HEAD : HEAD + 1])).T.astype(BF)

        for t in range(len(items) + 2):
            if t < len(items):
                score(t)
            if 0 <= t - 1 < len(items):
                weigh(t - 1)
            if 0 <= t - 2 < len(items):
                mix(t - 2)

    def group(g, _):
        slot = lax.rem(g, 2)
        for c in load(g):
            c.wait()

        @pl.when(g < 3)
        def _():
            for c in load(g + 1):
                c.start()

        @pl.when(g >= 2)
        def _():
            here, there = leave(g - 2)
            here.wait()
            there.wait_send()

        @pl.when(chip == 0)
        def _():
            attention(slot, 2 * OWN)

        @pl.when(chip == 1)
        def _():
            attention(slot, 0)

        for c in leave(g):
            c.start()

    lax.fori_loop(0, 4, group, None)
    for g in (2, 3):
        here, there = leave(g)
        here.wait()
        there.wait_send()
    for g in range(4):
        leave(g)[1].wait_recv()


def attend(q, k, v):
    hbm = pl.BlockSpec(memory_space=pl.ANY)
    dma = pltpu.SemaphoreType.DMA
    return pl.pallas_call(
        _attend,
        in_specs=[hbm] * 3,
        out_specs=hbm,
        out_shape=jax.ShapeDtypeStruct((OWN, D), BF),
        scratch_shapes=[
            pltpu.VMEM((2, 2 * OWN, GROUP * HEAD), BF), pltpu.VMEM((2, 4 * OWN, HEAD), BF), pltpu.VMEM((2, HEAD, 4 * OWN), BF),
            pltpu.VMEM((2, 2 * OWN, GROUP * HEAD), BF),
            dma((2, 2)), dma((2, 2, 4)), dma((2,)), dma((4,)), dma((4,)),
        ],
        compiler_params=pltpu.CompilerParams(collective_id=1, has_side_effects=True, vmem_limit_bytes=62 * 2**20),
        cost_estimate=pl.CostEstimate(flops=24 * 1024 * 1536 * 512, bytes_accessed=16 * 2**20, transcendentals=24 * 1024 * 1536),
        name="attend",
    )(q, k, v)


def _out(x_ref, o_ref, w_ref, y_ref):
    y_ref[...] = (x_ref[...].astype(F32) + dot(o_ref[...], w_ref[...])).astype(BF)


def output(x, o, wo, bn=512):
    cols = pl.BlockSpec((OWN, bn), lambda j: (0, j))
    return pl.pallas_call(
        _out,
        grid=(D // bn,),
        in_specs=[cols, pl.BlockSpec((OWN, D), lambda j: (0, 0), pipeline_mode=pl.Buffered(1)), pl.BlockSpec((D, bn), lambda j: (0, j))],
        out_specs=cols,
        out_shape=jax.ShapeDtypeStruct((OWN, D), BF),
        compiler_params=pltpu.CompilerParams(dimension_semantics=("arbitrary",), vmem_limit_bytes=62 * 2**20),
        cost_estimate=pl.CostEstimate(flops=2 * OWN * D * D, bytes_accessed=2 * D * D + 6 * OWN * D, transcendentals=0),
        name="output",
    )(x, o, wo)


def solution(mesh):
    def step(x, gain, wq, wk, wv, wo):
        sp = lax.axis_index("sp")
        mate = sp + 1 - 2 * lax.rem(sp, 2)
        q, k, v = project(x, gain[None], *tables(sp * OWN, mate * OWN), wq, wk, wv)
        return output(x, attend(q, k, v), wo)

    tokens, whole = P(("dp", "sp"), None), P(None, None)
    return jax.shard_map(
        step,
        mesh=mesh,
        in_specs=(tokens, P(None), whole, whole, whole, whole),
        out_specs=tokens,
        check_vma=False,
    )
```

```python
import functools

import jax
import jax.numpy as jnp
from jax import lax
from jax.experimental import pallas as pl
from jax.experimental.pallas import tpu as pltpu
from jax.sharding import PartitionSpec as P

HEAD = 128
THETA = 10000
NEG = -1e30
HIDDEN = 2 * NEG
E2 = HEAD**-0.5 * 1.4426950408889634
OWN = 512
D = 6144
HALF = 3072
KVH = 512
BF, F32 = jnp.bfloat16, jnp.float32


def dot(a, b, ca=1, cb=0):
    return lax.dot_general(a, b, (((ca,), (cb,)), ((), ())), preferred_element_type=F32)


def turn(t, cos, sin):
    return (t * cos + pltpu.roll(t, HEAD // 2, 1) * sin).astype(BF)


def tables(first, second):
    half = HEAD // 2
    column = jnp.arange(HEAD)
    place = (jnp.arange(OWN)[:, None] + jnp.where(column < half, first, second)).astype(F32)
    angle = place * THETA ** (-(column % half).astype(F32) / half)
    return jnp.cos(angle), jnp.sin(angle)


CHUNK = 128
TILE = 512
TILES = HALF // TILE
MESH = pl.DeviceIdType.MESH


def _project(x_hbm, g_ref, c_ref, s_ref, wq, wk, wv, q_hbm, k_hbm, v_hbm, xs, w, kv, qs, gain, cos, sin, xsem, xsend, xrecv, wsem, kvsem, ksend, krecv, qsem):
    sp = lax.axis_index("sp")
    core, chip = lax.rem(sp, 2), lax.div(sp, 2)
    mate, peer = sp + 1 - 2 * core, lax.rem(sp + 2, 4)

    def rows(i):
        return pl.ds(i * CHUNK, CHUNK)

    def weight(n):
        if isinstance(n, int) and n < 2:
            src = (wk, wv)[n].at[:, pl.ds(pl.multiple_of(core * KVH, KVH), KVH)]
        else:
            src = wq.at[:, pl.ds(pl.multiple_of(core * HALF + (n - 2) * TILE, TILE), TILE)]
        slot = lax.rem(n, 4)
        return pltpu.make_async_copy(src, w.at[slot], wsem.at[slot])

    mine = [pltpu.make_async_copy(x_hbm.at[rows(i)], xs.at[rows(i)], xsem.at[i]) for i in range(OWN // CHUNK)]
    for c in mine:
        c.start()
    barrier = pltpu.get_barrier_semaphore()
    for other in (mate, peer):
        pl.semaphore_signal(barrier, inc=1, device_id={"sp": other}, device_id_type=MESH)
    pl.semaphore_wait(barrier, 2)
    swaps = [
        pltpu.make_async_remote_copy(
            src_ref=x_hbm.at[pl.ds(i * OWN // 2, OWN // 2)], dst_ref=xs.at[pl.ds(OWN + i * OWN // 2, OWN // 2)],
            send_sem=xsend.at[i], recv_sem=xrecv.at[i], device_id={"sp": mate}, device_id_type=MESH)
        for i in range(2)
    ]
    for c in swaps:
        c.start()
    gain[...] = g_ref[...].astype(F32)
    half = HEAD // 2
    for b, part in enumerate((slice(0, half), slice(half, HEAD))):
        cos[b * OWN : (b + 1) * OWN, :] = jnp.concatenate([c_ref[:, part], c_ref[:, part]], 1)
        sin[b * OWN : (b + 1) * OWN, :] = jnp.concatenate([-s_ref[:, part], s_ref[:, part]], 1)

    def norm(at, n):
        wide = xs[pl.ds(at, n), :].astype(F32)
        scale = lax.rsqrt(jnp.mean(wide * wide, -1, keepdims=True) + 1e-6)
        xs[pl.ds(at, n), :] = (wide * scale * gain[...]).astype(BF)

    def turned_to(dst, t, at):
        n = t.shape[0]
        t = t.astype(BF).astype(F32)
        for h in range(TILE // HEAD):
            one = slice(h * HEAD, (h + 1) * HEAD)
            dst[:, one] = turn(t[:, one], cos[pl.ds(at, n), :], sin[pl.ds(at, n), :])

    def leave(s, p):
        block, n = lax.rem(core + s, 2), 2 * s + p
        out = (k_hbm, v_hbm)[p]
        return (
            pltpu.make_async_copy(kv.at[n], out.at[2 + block], kvsem.at[n]),
            pltpu.make_async_remote_copy(
                src_ref=kv.at[n], dst_ref=out.at[block], send_sem=ksend.at[n], recv_sem=krecv.at[n],
                device_id={"sp": peer}, device_id_type=MESH),
        )

    def send(s, p):
        here, there = leave(s, p)
        here.start()

        @pl.when(chip == 0)
        def _():
            there.start()

    def q_out(tile, s):
        cols = pl.ds(pl.multiple_of(tile * TILE, TILE), TILE)
        part = lax.rem(tile, 2)
        return pltpu.make_async_copy(qs.at[part, pl.ds(s * OWN, OWN)], q_hbm.at[lax.rem(core + s, 2), :, cols], qsem.at[part, s])

    def normed(at, n):
        for r in range(at, at + n, 32):
            norm(r, 32)

    def keys(at, n):
        set_ = at // OWN
        turned_to(kv.at[2 * set_, pl.ds(at - set_ * OWN, n)], dot(xs[at : at + n, :], w[0]), at)

    def values(set_):
        return dot(xs[set_ * OWN : (set_ + 1) * OWN, :], w[1]).T.astype(BF)

    half = OWN // 2
    mine[0].wait()
    weight(0).start()
    for i in range(2):
        if i:
            mine[i].wait()
        lax.fori_loop(0, CHUNK // 32, lambda r, _: norm(pl.multiple_of(i * CHUNK + r * 32, 32), 32), None)
    mine[2].wait()
    mine[3].wait()
    weight(1).start()
    weight(0).wait()
    keys(0, half)
    normed(half, half)
    keys(half, half)
    send(0, 0)
    weight(1).wait()
    weight(2).start()
    swaps[0].wait_recv()
    kv[1] = values(0)
    normed(OWN, half)
    send(0, 1)
    swaps[1].wait_recv()
    weight(3).start()
    keys(OWN, half)
    normed(OWN + half, half)
    keys(OWN + half, half)
    send(1, 0)
    weight(2).wait()
    weight(4).start()
    kv[3] = values(1)
    send(1, 1)
    weight(5).start()

    def tile(t, _):
        @pl.when(t < TILES - 1)
        def _():
            weight(t + 3).wait()

        @pl.when(t >= 2)
        def _():
            for s in range(2):
                q_out(t - 2, s).wait()

        turned_to(qs.at[lax.rem(t, 2)], dot(xs[...], w[lax.rem(t + 2, 4)]), 0)
        for s in range(2):
            q_out(t, s).start()

        @pl.when(t < TILES - 4)
        def _():
            weight(t + 6).start()

    lax.fori_loop(0, TILES, tile, None)
    for t in (TILES - 2, TILES - 1):
        for s in range(2):
            q_out(t, s).wait()
    for c in swaps:
        c.wait_send()
    for s in range(2):
        for p in range(2):
            here, there = leave(s, p)
            here.wait()

            @pl.when(chip == 0)
            def _():
                there.wait_send()

            @pl.when(chip == 1)
            def _():
                there.wait_recv()


def project(x, gain, cos, sin, wq, wk, wv):
    vmem, hbm = pl.BlockSpec(memory_space=pltpu.VMEM), pl.BlockSpec(memory_space=pl.ANY)
    dma = pltpu.SemaphoreType.DMA
    return pl.pallas_call(
        _project,
        in_specs=[hbm, vmem, vmem, vmem, hbm, hbm, hbm],
        out_specs=[hbm] * 3,
        out_shape=[
            jax.ShapeDtypeStruct((2, OWN, HALF), BF),
            jax.ShapeDtypeStruct((4, OWN, KVH), BF),
            jax.ShapeDtypeStruct((4, KVH, OWN), BF),
        ],
        scratch_shapes=[
            pltpu.VMEM((2 * OWN, D), BF), pltpu.VMEM((4, D, TILE), BF), pltpu.VMEM((4, OWN, KVH), BF), pltpu.VMEM((2, 2 * OWN, TILE), BF),
            pltpu.VMEM((1, D), F32), pltpu.VMEM((2 * OWN, HEAD), F32), pltpu.VMEM((2 * OWN, HEAD), F32),
            dma((4,)), dma((2,)), dma((2,)), dma((4,)), dma((4,)), dma((4,)), dma((4,)), dma((2, 2)),
        ],
        compiler_params=pltpu.CompilerParams(collective_id=0, has_side_effects=True, vmem_limit_bytes=62 * 2**20),
        cost_estimate=pl.CostEstimate(flops=4 * OWN * D * (HALF + 2 * KVH), bytes_accessed=2 * D * (HALF + 2 * KVH) + 8 * OWN * D, transcendentals=0),
        name="project",
    )(x, gain, cos, sin, wq, wk, wv)


GROUP = 6
STRIP = 256


def _attend(q_hbm, k_hbm, v_hbm, out, q, k, v, o, qsem, ksem, osend, orecv):
    sp = lax.axis_index("sp")
    core, chip = lax.rem(sp, 2), lax.div(sp, 2)
    mate = sp + 1 - 2 * core

    def load(g):
        slot = lax.rem(g, 2)
        wide, one = pl.ds(pl.multiple_of(g * GROUP * HEAD, HEAD), GROUP * HEAD), pl.ds(pl.multiple_of(g * HEAD, HEAD), HEAD)
        return (
            [pltpu.make_async_copy(q_hbm.at[b, :, wide], q.at[slot, pl.ds(b * OWN, OWN)], qsem.at[slot, b]) for b in range(2)]
            + [pltpu.make_async_copy(k_hbm.at[b, :, one], k.at[slot, pl.ds(b * OWN, OWN)], ksem.at[slot, 0, b]) for b in range(4)]
            + [pltpu.make_async_copy(v_hbm.at[b, one, :], v.at[slot, :, pl.ds(b * OWN, OWN)], ksem.at[slot, 1, b]) for b in range(4)]
        )

    def columns(g):
        return pl.ds(pl.multiple_of(core * HALF + g * GROUP * HEAD, HEAD), GROUP * HEAD)

    def tokens(c):
        return pl.ds(pl.multiple_of(c * OWN, OWN), OWN)

    def leave(g):
        return pltpu.make_async_remote_copy(
            src_ref=o.at[lax.rem(g, 2), tokens(1 - core)], dst_ref=out.at[:, columns(g)], send_sem=osend.at[g], recv_sem=orecv.at[g],
            device_id={"sp": mate}, device_id_type=MESH)

    for c in load(0):
        c.start()
    barrier = pltpu.get_barrier_semaphore()
    pl.semaphore_signal(barrier, inc=1, device_id={"sp": mate}, device_id_type=MESH)
    pl.semaphore_wait(barrier, 1)

    def attention(slot, first):
        items = [(h, i) for h in range(GROUP) for i in range(2 * OWN // STRIP)]
        scores, weights = {}, {}

        def end(i):
            return 2 * OWN + (i + 1) * STRIP

        def score(t):
            h, i = items[t]
            queries = q[slot, i * STRIP : (i + 1) * STRIP, h * HEAD : (h + 1) * HEAD]
            scores[t] = [dot(k[slot, a : a + STRIP, :], queries, 1, 1) for a in range(first, end(i), STRIP)]

        def weigh(t):
            s = scores.pop(t)
            ok = lax.broadcasted_iota(jnp.int32, (STRIP, STRIP), 0) <= lax.broadcasted_iota(jnp.int32, (STRIP, STRIP), 1)
            s = s[:-1] + [jnp.where(ok, s[-1], HIDDEN)]
            top = functools.reduce(jnp.maximum, [x.max(axis=0, keepdims=True) for x in s])
            weights[t] = [jnp.exp2((x - top) * E2).astype(BF) for x in s]

        def mix(t):
            h, i = items[t]
            values = jnp.concatenate([v[slot, :, first : end(i)], jnp.ones((16, end(i) - first), BF)], 0)
            m = dot(values, jnp.concatenate(weights.pop(t), 0))
            o[slot, i * STRIP : (i + 1) * STRIP, h * HEAD : (h + 1) * HEAD] = (m[:HEAD] * (1 / m[HEAD : HEAD + 1])).T.astype(BF)

        for t in range(len(items) + 2):
            if t < len(items):
                score(t)
            if 0 <= t - 1 < len(items):
                weigh(t - 1)
            if 0 <= t - 2 < len(items):
                mix(t - 2)

    def group(g, _):
        slot = lax.rem(g, 2)
        for c in load(g):
            c.wait()

        @pl.when(g < 3)
        def _():
            for c in load(g + 1):
                c.start()

        @pl.when(g >= 2)
        def _():
            leave(g - 2).wait_send()

        @pl.when(chip == 0)
        def _():
            attention(slot, 2 * OWN)

        @pl.when(chip == 1)
        def _():
            attention(slot, 0)

        leave(g).start()
        out[:, columns(g)] = o[slot, tokens(core)]

    lax.fori_loop(0, 4, group, None)
    for g in (2, 3):
        leave(g).wait_send()
    for g in range(4):
        leave(g).wait_recv()


def attend(q, k, v):
    hbm = pl.BlockSpec(memory_space=pl.ANY)
    dma = pltpu.SemaphoreType.DMA
    return pl.pallas_call(
        _attend,
        in_specs=[hbm] * 3,
        out_specs=pl.BlockSpec(memory_space=pltpu.VMEM),
        out_shape=pltpu.VMEM((OWN, D), BF),
        scratch_shapes=[
            pltpu.VMEM((2, 2 * OWN, GROUP * HEAD), BF), pltpu.VMEM((2, 4 * OWN, HEAD), BF), pltpu.VMEM((2, HEAD, 4 * OWN), BF),
            pltpu.VMEM((2, 2 * OWN, GROUP * HEAD), BF),
            dma((2, 2)), dma((2, 2, 4)), dma((4,)), dma((4,)),
        ],
        compiler_params=pltpu.CompilerParams(collective_id=1, has_side_effects=True, vmem_limit_bytes=50 * 2**20),
        cost_estimate=pl.CostEstimate(flops=24 * 1024 * 1536 * 512, bytes_accessed=16 * 2**20, transcendentals=24 * 1024 * 1536),
        name="attend",
    )(q, k, v)


def _out(x_ref, o_ref, w_ref, y_ref):
    y_ref[...] = (x_ref[...].astype(F32) + dot(o_ref[...], w_ref[...])).astype(BF)


def output(x, o, wo, bn=512):
    cols = pl.BlockSpec((OWN, bn), lambda j: (0, j))
    return pl.pallas_call(
        _out,
        grid=(D // bn,),
        in_specs=[cols, pl.BlockSpec(memory_space=pltpu.VMEM), pl.BlockSpec((D, bn), lambda j: (0, j))],
        out_specs=cols,
        out_shape=jax.ShapeDtypeStruct((OWN, D), BF),
        compiler_params=pltpu.CompilerParams(dimension_semantics=("arbitrary",), vmem_limit_bytes=50 * 2**20),
        cost_estimate=pl.CostEstimate(flops=2 * OWN * D * D, bytes_accessed=2 * D * D + 6 * OWN * D, transcendentals=0),
        name="output",
    )(x, o, wo)


def solution(mesh):
    def step(x, gain, wq, wk, wv, wo):
        sp = lax.axis_index("sp")
        mate = sp + 1 - 2 * lax.rem(sp, 2)
        q, k, v = project(x, gain[None], *tables(sp * OWN, mate * OWN), wq, wk, wv)
        return output(x, pltpu.with_memory_space_constraint(attend(q, k, v), pltpu.VMEM), wo)

    tokens, whole = P(("dp", "sp"), None), P(None, None)
    return jax.shard_map(
        step,
        mesh=mesh,
        in_specs=(tokens, P(None), whole, whole, whole, whole),
        out_specs=tokens,
        check_vma=False,
    )
```

```python
import functools

import jax
import jax.numpy as jnp
from jax import lax
from jax.experimental import pallas as pl
from jax.experimental.pallas import tpu as pltpu
from jax.sharding import PartitionSpec as P

HEAD = 128
THETA = 10000
NEG = -1e30
HIDDEN = 2 * NEG
E2 = HEAD**-0.5 * 1.4426950408889634
OWN = 512
D = 6144
HALF = 3072
KVH = 512
BF, F32 = jnp.bfloat16, jnp.float32


def dot(a, b, ca=1, cb=0):
    return lax.dot_general(a, b, (((ca,), (cb,)), ((), ())), preferred_element_type=F32)


def turn(t, cos, sin):
    return (t * cos + pltpu.roll(t, HEAD // 2, 1) * sin).astype(BF)


def tables(first, second):
    half = HEAD // 2
    column = jnp.arange(HEAD)
    place = (jnp.arange(OWN)[:, None] + jnp.where(column < half, first, second)).astype(F32)
    angle = place * THETA ** (-(column % half).astype(F32) / half)
    return jnp.cos(angle), jnp.sin(angle)


CHUNK = 128
TILE = 512
TILES = HALF // TILE
MESH = pl.DeviceIdType.MESH


def _project(x_hbm, g_ref, c_ref, s_ref, wq, wk, wv, q_hbm, k_hbm, v_hbm, xs, w, kv, qs, gain, cos, sin, xsem, xsend, xrecv, wsem, kvsem, ksend, krecv, qsem):
    sp = lax.axis_index("sp")
    core, chip = lax.rem(sp, 2), lax.div(sp, 2)
    mate, peer = sp + 1 - 2 * core, lax.rem(sp + 2, 4)

    def rows(i):
        return pl.ds(i * CHUNK, CHUNK)

    def weight(n):
        if isinstance(n, int) and n < 2:
            src = (wk, wv)[n].at[:, pl.ds(pl.multiple_of(core * KVH, KVH), KVH)]
        else:
            src = wq.at[:, pl.ds(pl.multiple_of(core * HALF + (n - 2) * TILE, TILE), TILE)]
        slot = lax.rem(n, 4)
        return pltpu.make_async_copy(src, w.at[slot], wsem.at[slot])

    mine = [pltpu.make_async_copy(x_hbm.at[rows(i)], xs.at[rows(i)], xsem.at[i]) for i in range(OWN // CHUNK)]
    for c in mine:
        c.start()
    barrier = pltpu.get_barrier_semaphore()
    for other in (mate, peer):
        pl.semaphore_signal(barrier, inc=1, device_id={"sp": other}, device_id_type=MESH)
    pl.semaphore_wait(barrier, 2)
    swaps = [
        pltpu.make_async_remote_copy(
            src_ref=xs.at[rows(i)], dst_ref=xs.at[pl.ds(OWN + i * CHUNK, CHUNK)], send_sem=xsend.at[i], recv_sem=xrecv.at[i],
            device_id={"sp": mate}, device_id_type=MESH)
        for i in range(OWN // CHUNK)
    ]
    gain[...] = g_ref[...].astype(F32).reshape(1, D)
    half = HEAD // 2
    for b, part in enumerate((slice(0, half), slice(half, HEAD))):
        cos[b * OWN : (b + 1) * OWN, :] = jnp.concatenate([c_ref[:, part], c_ref[:, part]], 1)
        sin[b * OWN : (b + 1) * OWN, :] = jnp.concatenate([-s_ref[:, part], s_ref[:, part]], 1)

    def norm(at, n):
        wide = xs[pl.ds(at, n), :].astype(F32)
        scale = lax.rsqrt(jnp.mean(wide * wide, -1, keepdims=True) + 1e-6)
        xs[pl.ds(at, n), :] = (wide * scale * gain[...]).astype(BF)

    def turned_to(dst, t, at):
        n = t.shape[0]
        t = t.astype(BF).astype(F32)
        for h in range(TILE // HEAD):
            one = slice(h * HEAD, (h + 1) * HEAD)
            dst[:, one] = turn(t[:, one], cos[pl.ds(at, n), :], sin[pl.ds(at, n), :])

    def leave(s, p):
        block, n = lax.rem(core + s, 2), 2 * s + p
        out = (k_hbm, v_hbm)[p]
        return (
            pltpu.make_async_copy(kv.at[n], out.at[2 + block], kvsem.at[n]),
            pltpu.make_async_remote_copy(
                src_ref=kv.at[n], dst_ref=out.at[block], send_sem=ksend.at[n], recv_sem=krecv.at[n],
                device_id={"sp": peer}, device_id_type=MESH),
        )

    def send(s, p):
        here, there = leave(s, p)
        here.start()

        @pl.when(chip == 0)
        def _():
            there.start()

    def q_out(tile, s):
        cols = pl.ds(pl.multiple_of(tile * TILE, TILE), TILE)
        part = lax.rem(tile, 2)
        return pltpu.make_async_copy(qs.at[part, pl.ds(s * OWN, OWN)], q_hbm.at[lax.rem(core + s, 2), :, cols], qsem.at[part, s])

    def keys(set_):
        turned_to(kv.at[2 * set_], dot(xs[set_ * OWN : (set_ + 1) * OWN, :], w[0]), set_ * OWN)
        send(set_, 0)

    def values(set_):
        kv[2 * set_ + 1] = dot(xs[set_ * OWN : (set_ + 1) * OWN, :], w[1]).T.astype(BF)
        send(set_, 1)

    for i in range(OWN // CHUNK):
        mine[i].wait()
        if i < 2:
            weight(i).start()
        lax.fori_loop(0, CHUNK // 32, lambda r, _: norm(pl.multiple_of(i * CHUNK + r * 32, 32), 32), None)
        swaps[i].start()
    weight(0).wait()
    keys(0)
    weight(1).wait()
    weight(2).start()
    values(0)
    weight(3).start()
    for c in swaps:
        c.wait_recv()
    keys(1)
    weight(2).wait()
    weight(4).start()
    values(1)
    weight(5).start()

    def tile(t, _):
        @pl.when(t < TILES - 1)
        def _():
            weight(t + 3).wait()

        @pl.when(t >= 2)
        def _():
            for s in range(2):
                q_out(t - 2, s).wait()

        turned_to(qs.at[lax.rem(t, 2)], dot(xs[...], w[lax.rem(t + 2, 4)]), 0)
        for s in range(2):
            q_out(t, s).start()

        @pl.when(t < TILES - 4)
        def _():
            weight(t + 6).start()

    lax.fori_loop(0, TILES, tile, None)
    for t in (TILES - 2, TILES - 1):
        for s in range(2):
            q_out(t, s).wait()
    for c in swaps:
        c.wait_send()
    for s in range(2):
        for p in range(2):
            here, there = leave(s, p)
            here.wait()

            @pl.when(chip == 0)
            def _():
                there.wait_send()

            @pl.when(chip == 1)
            def _():
                there.wait_recv()


def project(x, gain, cos, sin, wq, wk, wv):
    vmem, hbm = pl.BlockSpec(memory_space=pltpu.VMEM), pl.BlockSpec(memory_space=pl.ANY)
    dma = pltpu.SemaphoreType.DMA
    return pl.pallas_call(
        _project,
        in_specs=[hbm, vmem, vmem, vmem, hbm, hbm, hbm],
        out_specs=[hbm] * 3,
        out_shape=[
            jax.ShapeDtypeStruct((2, OWN, HALF), BF),
            jax.ShapeDtypeStruct((4, OWN, KVH), BF),
            jax.ShapeDtypeStruct((4, KVH, OWN), BF),
        ],
        scratch_shapes=[
            pltpu.VMEM((2 * OWN, D), BF), pltpu.VMEM((4, D, TILE), BF), pltpu.VMEM((4, OWN, KVH), BF), pltpu.VMEM((2, 2 * OWN, TILE), BF),
            pltpu.VMEM((1, D), F32), pltpu.VMEM((2 * OWN, HEAD), F32), pltpu.VMEM((2 * OWN, HEAD), F32),
            dma((4,)), dma((4,)), dma((4,)), dma((4,)), dma((4,)), dma((4,)), dma((4,)), dma((2, 2)),
        ],
        compiler_params=pltpu.CompilerParams(collective_id=0, has_side_effects=True, vmem_limit_bytes=62 * 2**20),
        cost_estimate=pl.CostEstimate(flops=4 * OWN * D * (HALF + 2 * KVH), bytes_accessed=2 * D * (HALF + 2 * KVH) + 8 * OWN * D, transcendentals=0),
        name="project",
    )(x, gain, cos, sin, wq, wk, wv)


GROUP = 6
STRIP = 256


def _attend(q_hbm, k_hbm, v_hbm, wo, out, w0, q, k, v, o, qsem, ksem, osend, orecv, wsem):
    sp = lax.axis_index("sp")
    core, chip = lax.rem(sp, 2), lax.div(sp, 2)
    mate = sp + 1 - 2 * core

    def load(g):
        slot = lax.rem(g, 2)
        wide, one = pl.ds(pl.multiple_of(g * GROUP * HEAD, HEAD), GROUP * HEAD), pl.ds(pl.multiple_of(g * HEAD, HEAD), HEAD)
        return (
            [pltpu.make_async_copy(q_hbm.at[b, :, wide], q.at[slot, pl.ds(b * OWN, OWN)], qsem.at[slot, b]) for b in range(2)]
            + [pltpu.make_async_copy(k_hbm.at[b, :, one], k.at[slot, pl.ds(b * OWN, OWN)], ksem.at[slot, 0, b]) for b in range(4)]
            + [pltpu.make_async_copy(v_hbm.at[b, one, :], v.at[slot, :, pl.ds(b * OWN, OWN)], ksem.at[slot, 1, b]) for b in range(4)]
        )

    def columns(g):
        return pl.ds(pl.multiple_of(core * HALF + g * GROUP * HEAD, HEAD), GROUP * HEAD)

    def tokens(c):
        return pl.ds(pl.multiple_of(c * OWN, OWN), OWN)

    def leave(g):
        return pltpu.make_async_remote_copy(
            src_ref=o.at[lax.rem(g, 2), tokens(1 - core)], dst_ref=out.at[:, columns(g)], send_sem=osend.at[g], recv_sem=orecv.at[g],
            device_id={"sp": mate}, device_id_type=MESH)

    for c in load(0):
        c.start()
    first_weights = pltpu.make_async_copy(wo.at[:, pl.ds(0, TILE)], w0, wsem)
    first_weights.start()
    barrier = pltpu.get_barrier_semaphore()
    pl.semaphore_signal(barrier, inc=1, device_id={"sp": mate}, device_id_type=MESH)
    pl.semaphore_wait(barrier, 1)

    def attention(slot, first):
        items = [(h, i) for h in range(GROUP) for i in range(2 * OWN // STRIP)]
        scores, weights = {}, {}

        def end(i):
            return 2 * OWN + (i + 1) * STRIP

        def score(t):
            h, i = items[t]
            queries = q[slot, i * STRIP : (i + 1) * STRIP, h * HEAD : (h + 1) * HEAD]
            scores[t] = [dot(k[slot, a : a + STRIP, :], queries, 1, 1) for a in range(first, end(i), STRIP)]

        def weigh(t):
            s = scores.pop(t)
            ok = lax.broadcasted_iota(jnp.int32, (STRIP, STRIP), 0) <= lax.broadcasted_iota(jnp.int32, (STRIP, STRIP), 1)
            s = s[:-1] + [jnp.where(ok, s[-1], HIDDEN)]
            top = functools.reduce(jnp.maximum, [x.max(axis=0, keepdims=True) for x in s])
            weights[t] = [jnp.exp2((x - top) * E2).astype(BF) for x in s]

        def mix(t):
            h, i = items[t]
            values = jnp.concatenate([v[slot, :, first : end(i)], jnp.ones((16, end(i) - first), BF)], 0)
            m = dot(values, jnp.concatenate(weights.pop(t), 0))
            o[slot, i * STRIP : (i + 1) * STRIP, h * HEAD : (h + 1) * HEAD] = (m[:HEAD] * (1 / m[HEAD : HEAD + 1])).T.astype(BF)

        for t in range(len(items) + 2):
            if t < len(items):
                score(t)
            if 0 <= t - 1 < len(items):
                weigh(t - 1)
            if 0 <= t - 2 < len(items):
                mix(t - 2)

    def group(g, _):
        slot = lax.rem(g, 2)
        for c in load(g):
            c.wait()

        @pl.when(g < 3)
        def _():
            for c in load(g + 1):
                c.start()

        @pl.when(g >= 2)
        def _():
            leave(g - 2).wait_send()

        @pl.when(chip == 0)
        def _():
            attention(slot, 2 * OWN)

        @pl.when(chip == 1)
        def _():
            attention(slot, 0)

        leave(g).start()
        out[:, columns(g)] = o[slot, tokens(core)]

    lax.fori_loop(0, 4, group, None)
    for g in (2, 3):
        leave(g).wait_send()
    for g in range(4):
        leave(g).wait_recv()
    first_weights.wait()


def attend(q, k, v, wo):
    hbm = pl.BlockSpec(memory_space=pl.ANY)
    dma = pltpu.SemaphoreType.DMA
    return pl.pallas_call(
        _attend,
        in_specs=[hbm] * 4,
        out_specs=[pl.BlockSpec(memory_space=pltpu.VMEM)] * 2,
        out_shape=[pltpu.VMEM((OWN, D), BF), pltpu.VMEM((D, TILE), BF)],
        scratch_shapes=[
            pltpu.VMEM((2, 2 * OWN, GROUP * HEAD), BF), pltpu.VMEM((2, 4 * OWN, HEAD), BF), pltpu.VMEM((2, HEAD, 4 * OWN), BF),
            pltpu.VMEM((2, 2 * OWN, GROUP * HEAD), BF),
            dma((2, 2)), dma((2, 2, 4)), dma((4,)), dma((4,)), dma,
        ],
        compiler_params=pltpu.CompilerParams(collective_id=1, has_side_effects=True, vmem_limit_bytes=44 * 2**20),
        cost_estimate=pl.CostEstimate(flops=24 * 1024 * 1536 * 512, bytes_accessed=16 * 2**20, transcendentals=24 * 1024 * 1536),
        name="attend",
    )(q, k, v, wo)


def _out(x_hbm, o, w0, wo, y_hbm, x, w, y, xsem, wsem, ysem):
    tiles = D // TILE

    def cols(t):
        return pl.ds(pl.multiple_of(t * TILE, TILE), TILE)

    def weight(t):
        slot = lax.rem(t, 3)
        return pltpu.make_async_copy(wo.at[:, cols(t)], w.at[slot], wsem.at[slot])

    def residual(t):
        return pltpu.make_async_copy(x_hbm.at[:, cols(t)], x.at[t], xsem.at[t])

    def leave(t):
        slot = lax.rem(t, 2)
        return pltpu.make_async_copy(y.at[slot], y_hbm.at[:, cols(t)], ysem.at[slot])

    residual(0).start()
    weight(1).start()
    weight(2).start()
    for t in range(1, tiles):
        residual(t).start()
    weight(3).start()
    product = dot(o[...], w0[...])
    residual(0).wait()
    y[0] = (x[0].astype(F32) + product).astype(BF)
    leave(0).start()
    weight(1).wait()

    def tile(t, _):
        @pl.when(t < tiles - 1)
        def _():
            weight(t + 1).wait()

        residual(t).wait()

        @pl.when(t >= 2)
        def _():
            leave(t - 2).wait()

        y[lax.rem(t, 2)] = (x[t].astype(F32) + dot(o[...], w[lax.rem(t, 3)])).astype(BF)
        leave(t).start()

        @pl.when(t < tiles - 3)
        def _():
            weight(t + 3).start()

    lax.fori_loop(1, tiles, tile, None)
    leave(tiles - 2).wait()
    leave(tiles - 1).wait()


def output(x, o, w0, wo):
    vmem, hbm = pl.BlockSpec(memory_space=pltpu.VMEM), pl.BlockSpec(memory_space=pl.ANY)
    dma = pltpu.SemaphoreType.DMA
    return pl.pallas_call(
        _out,
        in_specs=[hbm, vmem, vmem, hbm],
        out_specs=hbm,
        out_shape=jax.ShapeDtypeStruct((OWN, D), BF),
        scratch_shapes=[
            pltpu.VMEM((D // TILE, OWN, TILE), BF), pltpu.VMEM((3, D, TILE), BF), pltpu.VMEM((2, OWN, TILE), BF),
            dma((D // TILE,)), dma((3,)), dma((2,)),
        ],
        compiler_params=pltpu.CompilerParams(vmem_limit_bytes=44 * 2**20),
        cost_estimate=pl.CostEstimate(flops=2 * OWN * D * D, bytes_accessed=2 * D * D + 6 * OWN * D, transcendentals=0),
        name="output",
    )(x, o, w0, wo)


def solution(mesh):
    def step(x, gain, wq, wk, wv, wo):
        sp = lax.axis_index("sp")
        mate = sp + 1 - 2 * lax.rem(sp, 2)
        q, k, v = project(x, gain, *tables(sp * OWN, mate * OWN), wq, wk, wv)
        o, w0 = (pltpu.with_memory_space_constraint(t, pltpu.VMEM) for t in attend(q, k, v, wo))
        return output(x, o, w0, wo)

    tokens, whole = P(("dp", "sp"), None), P(None, None)
    return jax.shard_map(
        step,
        mesh=mesh,
        in_specs=(tokens, P(None), whole, whole, whole, whole),
        out_specs=tokens,
        check_vma=False,
    )
```

```python
import functools

import jax
import jax.numpy as jnp
from jax import lax
from jax.experimental import pallas as pl
from jax.experimental.pallas import tpu as pltpu
from jax.sharding import PartitionSpec as P

HEAD = 128
THETA = 10000
NEG = -1e30
HIDDEN = 2 * NEG
E2 = HEAD**-0.5 * 1.4426950408889634
OWN = 512
D = 6144
HALF = 3072
KVH = 512
BF, F32 = jnp.bfloat16, jnp.float32


def dot(a, b, ca=1, cb=0):
    return lax.dot_general(a, b, (((ca,), (cb,)), ((), ())), preferred_element_type=F32)


def turn(t, cos, sin):
    return (t * cos + pltpu.roll(t, HEAD // 2, 1) * sin).astype(BF)


def tables(first, second):
    half = HEAD // 2
    column = jnp.arange(HEAD)
    place = (jnp.arange(OWN)[:, None] + jnp.where(column < half, first, second)).astype(F32)
    angle = place * THETA ** (-(column % half).astype(F32) / half)
    return jnp.cos(angle), jnp.sin(angle)


GROUP = 6
CHUNK = 128
TILE = 512
TILES = HALF // TILE
MESH = pl.DeviceIdType.MESH


def _project(x_hbm, g_ref, c_ref, s_ref, wq, wk, wv, q_hbm, k_hbm, v_hbm, r_hbm, xs, w, kv, qs, gain, cos, sin, xsem, xsend, xrecv, wsem, kvsem, ksend, krecv, qsem, rsend, rrecv):
    sp = lax.axis_index("sp")
    core, chip = lax.rem(sp, 2), lax.div(sp, 2)
    mate, peer = sp + 1 - 2 * core, lax.rem(sp + 2, 4)

    def rows(i):
        return pl.ds(i * CHUNK, CHUNK)

    def weight(n):
        if isinstance(n, int) and n < 2:
            src = (wk, wv)[n].at[:, pl.ds(pl.multiple_of(core * KVH, KVH), KVH)]
        else:
            src = wq.at[:, pl.ds(pl.multiple_of(core * HALF + (n - 2) * TILE, TILE), TILE)]
        slot = lax.rem(n, 4)
        return pltpu.make_async_copy(src, w.at[slot], wsem.at[slot])

    mine = [pltpu.make_async_copy(x_hbm.at[rows(i)], xs.at[rows(i)], xsem.at[i]) for i in range(OWN // CHUNK)]
    for c in mine:
        c.start()
    barrier = pltpu.get_barrier_semaphore()
    for other in (mate, peer):
        pl.semaphore_signal(barrier, inc=1, device_id={"sp": other}, device_id_type=MESH)
    pl.semaphore_wait(barrier, 2)
    swaps = [
        pltpu.make_async_remote_copy(
            src_ref=xs.at[rows(i)], dst_ref=xs.at[pl.ds(OWN + i * CHUNK, CHUNK)], send_sem=xsend.at[i], recv_sem=xrecv.at[i],
            device_id={"sp": mate}, device_id_type=MESH)
        for i in range(OWN // CHUNK)
    ]
    gain[...] = g_ref[...].astype(F32).reshape(1, D)
    half = HEAD // 2
    for b, part in enumerate((slice(0, half), slice(half, HEAD))):
        cos[b * OWN : (b + 1) * OWN, :] = jnp.concatenate([c_ref[:, part], c_ref[:, part]], 1)
        sin[b * OWN : (b + 1) * OWN, :] = jnp.concatenate([-s_ref[:, part], s_ref[:, part]], 1)

    def norm(at, n):
        wide = xs[pl.ds(at, n), :].astype(F32)
        scale = lax.rsqrt(jnp.mean(wide * wide, -1, keepdims=True) + 1e-6)
        xs[pl.ds(at, n), :] = (wide * scale * gain[...]).astype(BF)

    def turned_to(dst, t, at):
        n = t.shape[0]
        t = t.astype(BF).astype(F32)
        for h in range(TILE // HEAD):
            one = slice(h * HEAD, (h + 1) * HEAD)
            dst[:, one] = turn(t[:, one], cos[pl.ds(at, n), :], sin[pl.ds(at, n), :])

    def leave(s, p):
        block, n = lax.rem(core + s, 2), 2 * s + p
        out = (k_hbm, v_hbm)[p]
        rest = pl.ds(HEAD, KVH - HEAD)
        rest = (rest, slice(None)) if p else (slice(None), rest)
        return (
            pltpu.make_async_copy(kv.at[n], out.at[2 + block], kvsem.at[n]),
            pltpu.make_async_remote_copy(
                src_ref=kv.at[n, *rest], dst_ref=out.at[block, *rest], send_sem=ksend.at[n], recv_sem=krecv.at[n],
                device_id={"sp": peer}, device_id_type=MESH),
        )

    def send(s, p):
        here, there = leave(s, p)
        here.start()

        @pl.when(chip == 0)
        def _():
            there.start()

    def q_out(tile, s):
        cols = pl.ds(pl.multiple_of(tile * TILE, TILE), TILE)
        part = lax.rem(tile, 2)
        return pltpu.make_async_copy(qs.at[part, pl.ds(s * OWN, OWN)], q_hbm.at[lax.rem(core + s, 2), :, cols], qsem.at[part, s])

    def lend(t, s):
        block = lax.rem(core + s, 2)
        cols = pl.ds(t * TILE, TILE if t == 0 else GROUP * HEAD - TILE)
        return pltpu.make_async_remote_copy(
            src_ref=q_hbm.at[block, :, cols], dst_ref=r_hbm.at[block, :, cols], send_sem=rsend.at[t, s], recv_sem=rrecv.at[t, s],
            device_id={"sp": peer}, device_id_type=MESH)

    def keys(set_):
        turned_to(kv.at[2 * set_], dot(xs[set_ * OWN : (set_ + 1) * OWN, :], w[0]), set_ * OWN)
        send(set_, 0)

    def values(set_):
        kv[2 * set_ + 1] = dot(xs[set_ * OWN : (set_ + 1) * OWN, :], w[1]).T.astype(BF)
        send(set_, 1)

    for i in range(OWN // CHUNK):
        mine[i].wait()
        if i < 2:
            weight(i).start()
        lax.fori_loop(0, CHUNK // 32, lambda r, _: norm(pl.multiple_of(i * CHUNK + r * 32, 32), 32), None)
        swaps[i].start()
    weight(0).wait()
    keys(0)
    weight(1).wait()
    weight(2).start()
    values(0)
    weight(3).start()
    for c in swaps:
        c.wait_recv()
    keys(1)
    weight(2).wait()
    weight(4).start()
    values(1)
    weight(5).start()

    def tile(t, _):
        @pl.when(t < TILES - 1)
        def _():
            weight(t + 3).wait()

        @pl.when(t >= 4)
        def _():
            for s in range(2):
                q_out(t - 2, s).wait()

        turned_to(qs.at[lax.rem(t, 2)], dot(xs[...], w[lax.rem(t + 2, 4)]), 0)
        for s in range(2):
            q_out(t, s).start()

        @pl.when(t < TILES - 4)
        def _():
            weight(t + 6).start()

        for first in range(2):

            @pl.when(t == first)
            def _():
                for s in range(2):
                    q_out(first, s).wait()

                @pl.when(chip == 1)
                def _():
                    for s in range(2):
                        lend(first, s).start()

    lax.fori_loop(0, TILES, tile, None)
    for t in (TILES - 2, TILES - 1):
        for s in range(2):
            q_out(t, s).wait()
    for c in swaps:
        c.wait_send()
    for s in range(2):
        for t in range(2):

            @pl.when(chip == 1)
            def _():
                lend(t, s).wait_send()

            @pl.when(chip == 0)
            def _():
                lend(t, s).wait_recv()

        for p in range(2):
            here, there = leave(s, p)
            here.wait()

            @pl.when(chip == 0)
            def _():
                there.wait_send()

            @pl.when(chip == 1)
            def _():
                there.wait_recv()


def project(x, gain, cos, sin, wq, wk, wv):
    vmem, hbm = pl.BlockSpec(memory_space=pltpu.VMEM), pl.BlockSpec(memory_space=pl.ANY)
    dma = pltpu.SemaphoreType.DMA
    return pl.pallas_call(
        _project,
        in_specs=[hbm, vmem, vmem, vmem, hbm, hbm, hbm],
        out_specs=[hbm] * 4,
        out_shape=[
            jax.ShapeDtypeStruct((2, OWN, HALF), BF),
            jax.ShapeDtypeStruct((4, OWN, KVH), BF),
            jax.ShapeDtypeStruct((4, KVH, OWN), BF),
            jax.ShapeDtypeStruct((2, OWN, GROUP * HEAD), BF),
        ],
        scratch_shapes=[
            pltpu.VMEM((2 * OWN, D), BF), pltpu.VMEM((4, D, TILE), BF), pltpu.VMEM((4, OWN, KVH), BF), pltpu.VMEM((2, 2 * OWN, TILE), BF),
            pltpu.VMEM((1, D), F32), pltpu.VMEM((2 * OWN, HEAD), F32), pltpu.VMEM((2 * OWN, HEAD), F32),
            dma((4,)), dma((4,)), dma((4,)), dma((4,)), dma((4,)), dma((4,)), dma((4,)), dma((2, 2)), dma((2, 2)), dma((2, 2)),
        ],
        compiler_params=pltpu.CompilerParams(collective_id=0, has_side_effects=True, vmem_limit_bytes=62 * 2**20),
        cost_estimate=pl.CostEstimate(flops=4 * OWN * D * (HALF + 2 * KVH), bytes_accessed=2 * D * (HALF + 2 * KVH) + 8 * OWN * D, transcendentals=0),
        name="project",
    )(x, gain, cos, sin, wq, wk, wv)


STRIP = 256


def _attend(q_hbm, k_hbm, v_hbm, r_hbm, wo, out, w0, q, k, v, o, part, found, other, qsem, ksem, osend, orecv, wsem, psend, precv, fsem):
    sp = lax.axis_index("sp")
    core, chip = lax.rem(sp, 2), lax.div(sp, 2)
    mate, peer = sp + 1 - 2 * core, lax.rem(sp + 2, 4)

    def load(g, slot, q_hbm=q_hbm):
        wide, one = pl.ds(pl.multiple_of(g * GROUP * HEAD, HEAD), GROUP * HEAD), pl.ds(pl.multiple_of(g * HEAD, HEAD), HEAD)
        return (
            [pltpu.make_async_copy(q_hbm.at[b, :, wide], q.at[slot, pl.ds(b * OWN, OWN)], qsem.at[slot, b]) for b in range(2)]
            + [pltpu.make_async_copy(k_hbm.at[b, :, one], k.at[slot, pl.ds(b * OWN, OWN)], ksem.at[slot, 0, b]) for b in range(4)]
            + [pltpu.make_async_copy(v_hbm.at[b, one, :], v.at[slot, :, pl.ds(b * OWN, OWN)], ksem.at[slot, 1, b]) for b in range(4)]
        )

    def columns(g):
        return pl.ds(pl.multiple_of(core * HALF + g * GROUP * HEAD, HEAD), GROUP * HEAD)

    def tokens(c):
        return pl.ds(pl.multiple_of(c * OWN, OWN), OWN)

    def leave(g):
        return pltpu.make_async_remote_copy(
            src_ref=o.at[lax.rem(g + 1, 2), tokens(1 - core)], dst_ref=out.at[:, columns(g)], send_sem=osend.at[g], recv_sem=orecv.at[g],
            device_id={"sp": mate}, device_id_type=MESH)

    for c in load(1, 0):
        c.start()
    lent = load(0, 1, r_hbm)

    @pl.when(chip == 0)
    def _():
        for c in lent:
            c.start()

    first_weights = pltpu.make_async_copy(wo.at[:, pl.ds(0, TILE)], w0, wsem)
    first_weights.start()
    barrier = pltpu.get_barrier_semaphore()
    for device in (mate, peer):
        pl.semaphore_signal(barrier, inc=1, device_id={"sp": device}, device_id_type=MESH)
    pl.semaphore_wait(barrier, 2)

    def give(p):
        two = pl.ds(2 * p, 2)
        return pltpu.make_async_remote_copy(
            src_ref=part.at[two], dst_ref=part.at[two], send_sem=psend.at[p], recv_sem=precv.at[p],
            device_id={"sp": peer}, device_id_type=MESH)

    give_found = pltpu.make_async_remote_copy(
        src_ref=found, dst_ref=other, send_sem=fsem.at[0], recv_sem=fsem.at[1], device_id={"sp": peer}, device_id_type=MESH)

    def attention(slot, first, lent=None):
        items = [(h, i) for h in range(GROUP if lent is None else 2) for i in range(2 * OWN // STRIP)]
        scores, weights = {}, {}

        def end(i):
            return 2 * OWN + (i + 1) * STRIP if lent is None else 4 * OWN

        def strip(i):
            return slice(i * STRIP, (i + 1) * STRIP)

        def score(t):
            h, i = items[t]
            head = slice(h * HEAD, (h + 1) * HEAD) if lent is None else pl.ds(pl.multiple_of((lent + h) * HEAD, HEAD), HEAD)
            queries = q[slot, strip(i), head]
            scores[t] = [dot(k[slot, a : a + STRIP, :], queries, 1, 1) for a in range(first, end(i), STRIP)]

        def weigh(t):
            s = scores.pop(t)
            if lent is None:
                ok = lax.broadcasted_iota(jnp.int32, (STRIP, STRIP), 0) <= lax.broadcasted_iota(jnp.int32, (STRIP, STRIP), 1)
                s = s[:-1] + [jnp.where(ok, s[-1], HIDDEN)]
            top = functools.reduce(jnp.maximum, [x.max(axis=0, keepdims=True) for x in s])
            weights[t] = [jnp.exp2((x - top) * E2).astype(BF) for x in s], top

        def mix(t):
            h, i = items[t]
            p, top = weights.pop(t)
            values = jnp.concatenate([v[slot, :, first : end(i)], jnp.ones((16, end(i) - first), BF)], 0)
            m = dot(values, jnp.concatenate(p, 0))
            total = m[HEAD : HEAD + 1]
            m = m[:HEAD] * (1 / total)
            if lent is not None:
                part[lent + h, :, strip(i)] = m.astype(BF)
                found[pl.ds(lent + h, 1), strip(i)] = top * E2 + jnp.log2(total)
                return
            if first:
                here, there = top * E2 + jnp.log2(total), other[h : h + 1, strip(i)]
                most = jnp.maximum(here, there)
                here, there = jnp.exp2(here - most), jnp.exp2(there - most)
                m = (m * here + part[h, :, strip(i)].astype(F32) * there) * (1 / (here + there))
            o[slot, strip(i), h * HEAD : (h + 1) * HEAD] = m.T.astype(BF)

        for t in range(len(items) + 2):
            if t < len(items):
                score(t)
            if 0 <= t - 1 < len(items):
                weigh(t - 1)
            if 0 <= t - 2 < len(items):
                mix(t - 2)

    @pl.when(chip == 0)
    def _():
        other[...] = jnp.full(other.shape, NEG, F32)
        for c in lent:
            c.wait()

        def two(p, _):
            attention(1, 2 * OWN, 2 * p)
            give(p).start()

        lax.fori_loop(0, GROUP // 2, two, None)
        give_found.start()

    def group(j, _):
        g, slot = lax.rem(j + 1, 4), lax.rem(j, 2)
        for c in load(g, slot):
            c.wait()

        @pl.when(j < 3)
        def _():
            for c in load(lax.rem(j + 2, 4), 1 - slot):
                c.start()

        @pl.when(j >= 2)
        def _():
            leave(j - 1).wait_send()

        @pl.when((chip == 1) & (j == 3))
        def _():
            for p in range(GROUP // 2):
                give(p).wait_recv()
            give_found.wait_recv()

        @pl.when((chip == 0) | (j == 3))
        def _():
            attention(slot, 2 * OWN)

        @pl.when((chip == 1) & (j < 3))
        def _():
            attention(slot, 0)

        leave(g).start()
        out[:, columns(g)] = o[slot, tokens(core)]

    lax.fori_loop(0, 4, group, None)
    for g in (3, 0):
        leave(g).wait_send()
    for g in range(4):
        leave(g).wait_recv()

    @pl.when(chip == 0)
    def _():
        for p in range(GROUP // 2):
            give(p).wait_send()
        give_found.wait_send()

    first_weights.wait()


def attend(q, k, v, r, wo):
    hbm = pl.BlockSpec(memory_space=pl.ANY)
    dma = pltpu.SemaphoreType.DMA
    return pl.pallas_call(
        _attend,
        in_specs=[hbm] * 5,
        out_specs=[pl.BlockSpec(memory_space=pltpu.VMEM)] * 2,
        out_shape=[pltpu.VMEM((OWN, D), BF), pltpu.VMEM((D, TILE), BF)],
        scratch_shapes=[
            pltpu.VMEM((2, 2 * OWN, GROUP * HEAD), BF), pltpu.VMEM((2, 4 * OWN, HEAD), BF), pltpu.VMEM((2, HEAD, 4 * OWN), BF),
            pltpu.VMEM((2, 2 * OWN, GROUP * HEAD), BF),
            pltpu.VMEM((GROUP, HEAD, 2 * OWN), BF), pltpu.VMEM((8, 2 * OWN), F32), pltpu.VMEM((8, 2 * OWN), F32),
            dma((2, 2)), dma((2, 2, 4)), dma((4,)), dma((4,)), dma, dma((3,)), dma((3,)), dma((2,)),
        ],
        compiler_params=pltpu.CompilerParams(collective_id=1, has_side_effects=True, vmem_limit_bytes=44 * 2**20),
        cost_estimate=pl.CostEstimate(flops=24 * 1024 * 1536 * 512, bytes_accessed=16 * 2**20, transcendentals=24 * 1024 * 1536),
        name="attend",
    )(q, k, v, r, wo)


def _out(x_hbm, o, w0, wo, y_hbm, x, w, y, xsem, wsem, ysem):
    tiles = D // TILE

    def cols(t):
        return pl.ds(pl.multiple_of(t * TILE, TILE), TILE)

    def weight(t):
        slot = lax.rem(t, 3)
        return pltpu.make_async_copy(wo.at[:, cols(t)], w.at[slot], wsem.at[slot])

    def residual(t):
        return pltpu.make_async_copy(x_hbm.at[:, cols(t)], x.at[t], xsem.at[t])

    def leave(t):
        slot = lax.rem(t, 2)
        return pltpu.make_async_copy(y.at[slot], y_hbm.at[:, cols(t)], ysem.at[slot])

    weight(1).start()
    residual(0).start()
    residual(1).start()
    weight(2).start()
    product = dot(o[...], w0[...])
    residual(0).wait()
    y[0] = (x[0].astype(F32) + product).astype(BF)
    leave(0).start()

    def tile(t, _):
        @pl.when(t == 1)
        def _():
            weight(1).wait()

        @pl.when(t < tiles - 1)
        def _():
            weight(t + 1).wait()
            residual(t + 1).start()

        residual(t).wait()

        @pl.when(t >= 2)
        def _():
            leave(t - 2).wait()

        @pl.when(t < tiles - 2)
        def _():
            weight(t + 2).start()

        y[lax.rem(t, 2)] = (x[t].astype(F32) + dot(o[...], w[lax.rem(t, 3)])).astype(BF)
        leave(t).start()

    lax.fori_loop(1, tiles, tile, None)
    leave(tiles - 2).wait()
    leave(tiles - 1).wait()


def output(x, o, w0, wo):
    vmem, hbm = pl.BlockSpec(memory_space=pltpu.VMEM), pl.BlockSpec(memory_space=pl.ANY)
    dma = pltpu.SemaphoreType.DMA
    return pl.pallas_call(
        _out,
        in_specs=[hbm, vmem, vmem, hbm],
        out_specs=hbm,
        out_shape=jax.ShapeDtypeStruct((OWN, D), BF),
        scratch_shapes=[
            pltpu.VMEM((D // TILE, OWN, TILE), BF), pltpu.VMEM((3, D, TILE), BF), pltpu.VMEM((2, OWN, TILE), BF),
            dma((D // TILE,)), dma((3,)), dma((2,)),
        ],
        compiler_params=pltpu.CompilerParams(vmem_limit_bytes=44 * 2**20),
        cost_estimate=pl.CostEstimate(flops=2 * OWN * D * D, bytes_accessed=2 * D * D + 6 * OWN * D, transcendentals=0),
        name="output",
    )(x, o, w0, wo)


def solution(mesh):
    def step(x, gain, wq, wk, wv, wo):
        sp = lax.axis_index("sp")
        mate = sp + 1 - 2 * lax.rem(sp, 2)
        q, k, v, r = project(x, gain, *tables(sp * OWN, mate * OWN), wq, wk, wv)
        o, w0 = (pltpu.with_memory_space_constraint(t, pltpu.VMEM) for t in attend(q, k, v, r, wo))
        return output(x, o, w0, wo)

    tokens, whole = P(("dp", "sp"), None), P(None, None)
    return jax.shard_map(
        step,
        mesh=mesh,
        in_specs=(tokens, P(None), whole, whole, whole, whole),
        out_specs=tokens,
        check_vma=False,
    )
```

```python
import functools

import jax
import jax.numpy as jnp
from jax import lax
from jax.experimental import pallas as pl
from jax.experimental.pallas import tpu as pltpu
from jax.sharding import PartitionSpec as P

HEAD = 128
THETA = 10000
NEG = -1e30
HIDDEN = 2 * NEG
E2 = HEAD**-0.5 * 1.4426950408889634
OWN = 512
RUN = 32
D = 6144
HALF = 3072
KVH = 512
BF, F32 = jnp.bfloat16, jnp.float32


def dot(a, b, ca=1, cb=0):
    return lax.dot_general(a, b, (((ca,), (cb,)), ((), ())), preferred_element_type=F32)


def turn(t, cos, sin):
    return (t * cos + pltpu.roll(t, HEAD // 2, 1) * sin).astype(BF)


def tables(first, second):
    half = HEAD // 2
    row = jnp.arange(2 * OWN // RUN + RUN)[:, None]
    n = OWN // RUN
    place = jnp.where(row < n, first + row * RUN, jnp.where(row < 2 * n, second + (row - n) * RUN, row - 2 * n)).astype(F32)
    angle = place * THETA ** (-(jnp.arange(HEAD) % half).astype(F32) / half)
    return jnp.cos(angle), jnp.sin(angle)


GROUP = 6
CHUNK = 128
TILE = 512
TILES = HALF // TILE
MESH = pl.DeviceIdType.MESH


def _project(x_hbm, g_ref, c_ref, s_ref, wq, wk, wv, q_hbm, k_hbm, v_hbm, r_hbm, xs, w, kv, qs, gain, cos, sin, xsem, xsend, xrecv, wsem, kvsem, ksend, krecv, qsem, rsend, rrecv):
    sp = lax.axis_index("sp")
    core, chip = lax.rem(sp, 2), lax.div(sp, 2)
    mate, peer = sp + 1 - 2 * core, lax.rem(sp + 2, 4)

    def rows(i):
        return pl.ds(i * CHUNK, CHUNK)

    def weight(n):
        if isinstance(n, int) and n < 2:
            src = (wk, wv)[n].at[:, pl.ds(pl.multiple_of(core * KVH, KVH), KVH)]
        else:
            src = wq.at[:, pl.ds(pl.multiple_of(core * HALF + (n - 2) * TILE, TILE), TILE)]
        slot = lax.rem(n, 4)
        return pltpu.make_async_copy(src, w.at[slot], wsem.at[slot])

    mine = [pltpu.make_async_copy(x_hbm.at[rows(i)], xs.at[rows(i)], xsem.at[i]) for i in range(OWN // CHUNK)]
    for c in mine:
        c.start()
    barrier = pltpu.get_barrier_semaphore()
    for other in (mate, peer):
        pl.semaphore_signal(barrier, inc=1, device_id={"sp": other}, device_id_type=MESH)
    pl.semaphore_wait(barrier, 2)
    swaps = [
        pltpu.make_async_remote_copy(
            src_ref=xs.at[rows(i)], dst_ref=xs.at[pl.ds(OWN + i * CHUNK, CHUNK)], send_sem=xsend.at[i], recv_sem=xrecv.at[i],
            device_id={"sp": mate}, device_id_type=MESH)
        for i in range(OWN // CHUNK)
    ]
    gain[...] = g_ref[...].astype(F32).reshape(1, D)
    coarse = 2 * OWN // RUN
    fine_c, fine_s = c_ref[coarse:, :], s_ref[coarse:, :]
    sign = jnp.where(lax.broadcasted_iota(jnp.int32, (1, HEAD), 1) < HEAD // 2, -1.0, 1.0)
    for n in range(coarse):
        c, s = c_ref[n : n + 1, :], s_ref[n : n + 1, :]
        cos[n * RUN : (n + 1) * RUN, :] = c * fine_c - s * fine_s
        sin[n * RUN : (n + 1) * RUN, :] = (s * sign) * fine_c + (c * sign) * fine_s

    def norm(at, n):
        wide = xs[pl.ds(at, n), :].astype(F32)
        scale = lax.rsqrt(jnp.mean(wide * wide, -1, keepdims=True) + 1e-6)
        xs[pl.ds(at, n), :] = (wide * scale * gain[...]).astype(BF)

    def turned_to(dst, t, at):
        n = t.shape[0]
        t = t.astype(BF).astype(F32)
        for h in range(TILE // HEAD):
            one = slice(h * HEAD, (h + 1) * HEAD)
            dst[:, one] = turn(t[:, one], cos[pl.ds(at, n), :], sin[pl.ds(at, n), :])

    def leave(s, p):
        block, n = lax.rem(core + s, 2), 2 * s + p
        out = (k_hbm, v_hbm)[p]
        rest = pl.ds(HEAD, KVH - HEAD)
        rest = (rest, slice(None)) if p else (slice(None), rest)
        return (
            pltpu.make_async_copy(kv.at[n], out.at[2 + block], kvsem.at[n]),
            pltpu.make_async_remote_copy(
                src_ref=kv.at[n, *rest], dst_ref=out.at[block, *rest], send_sem=ksend.at[n], recv_sem=krecv.at[n],
                device_id={"sp": peer}, device_id_type=MESH),
        )

    def send(s, p):
        here, there = leave(s, p)
        here.start()

        @pl.when(chip == 0)
        def _():
            there.start()

    def q_out(tile, s):
        cols = pl.ds(pl.multiple_of(tile * TILE, TILE), TILE)
        part = tile
        return pltpu.make_async_copy(qs.at[part, pl.ds(s * OWN, OWN)], q_hbm.at[lax.rem(core + s, 2), :, cols], qsem.at[part, s])

    def lend(t, s):
        block = lax.rem(core + s, 2)
        cols = pl.ds(t * TILE, TILE if t == 0 else GROUP * HEAD - TILE)
        return pltpu.make_async_remote_copy(
            src_ref=qs.at[t, pl.ds(s * OWN, OWN), pl.ds(0, cols.size)], dst_ref=r_hbm.at[block, :, cols], send_sem=rsend.at[t, s], recv_sem=rrecv.at[t, s],
            device_id={"sp": peer}, device_id_type=MESH)

    def keys(set_):
        turned_to(kv.at[2 * set_], dot(xs[set_ * OWN : (set_ + 1) * OWN, :], w[0]), set_ * OWN)
        send(set_, 0)

    def values(set_):
        kv[2 * set_ + 1] = dot(xs[set_ * OWN : (set_ + 1) * OWN, :], w[1]).T.astype(BF)
        send(set_, 1)

    for i in range(OWN // CHUNK):
        mine[i].wait()
        if i < 2:
            weight(i).start()
        lax.fori_loop(0, CHUNK // 32, lambda r, _: norm(pl.multiple_of(i * CHUNK + r * 32, 32), 32), None)
        swaps[i].start()
    weight(0).wait()
    keys(0)
    weight(1).wait()
    weight(2).start()
    values(0)
    weight(3).start()
    for c in swaps:
        c.wait_recv()
    keys(1)
    weight(2).wait()
    weight(4).start()
    values(1)
    weight(5).start()

    def tile(t, _):
        @pl.when(t < TILES - 1)
        def _():
            weight(t + 3).wait()

        turned_to(qs.at[t], dot(xs[...], w[lax.rem(t + 2, 4)]), 0)
        for s in range(2):
            q_out(t, s).start()

        @pl.when(t < TILES - 4)
        def _():
            weight(t + 6).start()

        for first in range(2):

            @pl.when((t == first) & (chip == 1))
            def _():
                for s in range(2):
                    lend(first, s).start()

    lax.fori_loop(0, TILES, tile, None)
    for t in range(TILES):
        for s in range(2):
            q_out(t, s).wait()
    for c in swaps:
        c.wait_send()
    for s in range(2):
        for t in range(2):

            @pl.when(chip == 1)
            def _():
                lend(t, s).wait_send()

            @pl.when(chip == 0)
            def _():
                lend(t, s).wait_recv()

        for p in range(2):
            here, there = leave(s, p)
            here.wait()

            @pl.when(chip == 0)
            def _():
                there.wait_send()

            @pl.when(chip == 1)
            def _():
                there.wait_recv()


def project(x, gain, cos, sin, wq, wk, wv):
    vmem, hbm = pl.BlockSpec(memory_space=pltpu.VMEM), pl.BlockSpec(memory_space=pl.ANY)
    dma = pltpu.SemaphoreType.DMA
    return pl.pallas_call(
        _project,
        in_specs=[hbm, vmem, vmem, vmem, hbm, hbm, hbm],
        out_specs=[hbm] * 4,
        out_shape=[
            jax.ShapeDtypeStruct((2, OWN, HALF), BF),
            jax.ShapeDtypeStruct((4, OWN, KVH), BF),
            jax.ShapeDtypeStruct((4, KVH, OWN), BF),
            jax.ShapeDtypeStruct((2, OWN, GROUP * HEAD), BF),
        ],
        scratch_shapes=[
            pltpu.VMEM((2 * OWN, D), BF), pltpu.VMEM((4, D, TILE), BF), pltpu.VMEM((4, OWN, KVH), BF), pltpu.VMEM((TILES, 2 * OWN, TILE), BF),
            pltpu.VMEM((1, D), F32), pltpu.VMEM((2 * OWN, HEAD), F32), pltpu.VMEM((2 * OWN, HEAD), F32),
            dma((4,)), dma((4,)), dma((4,)), dma((4,)), dma((4,)), dma((4,)), dma((4,)), dma((TILES, 2)), dma((2, 2)), dma((2, 2)),
        ],
        compiler_params=pltpu.CompilerParams(collective_id=0, has_side_effects=True, vmem_limit_bytes=62 * 2**20),
        cost_estimate=pl.CostEstimate(flops=4 * OWN * D * (HALF + 2 * KVH), bytes_accessed=2 * D * (HALF + 2 * KVH) + 8 * OWN * D, transcendentals=0),
        name="project",
    )(x, gain, cos, sin, wq, wk, wv)


STRIP = 256


def _attend(q_hbm, k_hbm, v_hbm, r_hbm, wo, out, w0, q, k, v, o, part, found, other, qsem, ksem, osend, orecv, wsem, psend, precv, fsem):
    sp = lax.axis_index("sp")
    core, chip = lax.rem(sp, 2), lax.div(sp, 2)
    mate, peer = sp + 1 - 2 * core, lax.rem(sp + 2, 4)

    def load(g, slot, q_hbm=q_hbm):
        wide, one = pl.ds(pl.multiple_of(g * GROUP * HEAD, HEAD), GROUP * HEAD), pl.ds(pl.multiple_of(g * HEAD, HEAD), HEAD)
        return (
            [pltpu.make_async_copy(q_hbm.at[b, :, wide], q.at[slot, pl.ds(b * OWN, OWN)], qsem.at[slot, b]) for b in range(2)]
            + [pltpu.make_async_copy(k_hbm.at[b, :, one], k.at[slot, pl.ds(b * OWN, OWN)], ksem.at[slot, 0, b]) for b in range(4)]
            + [pltpu.make_async_copy(v_hbm.at[b, one, :], v.at[slot, :, pl.ds(b * OWN, OWN)], ksem.at[slot, 1, b]) for b in range(4)]
        )

    def columns(g):
        return pl.ds(pl.multiple_of(core * HALF + g * GROUP * HEAD, HEAD), GROUP * HEAD)

    def tokens(c):
        return pl.ds(pl.multiple_of(c * OWN, OWN), OWN)

    def leave(g):
        return pltpu.make_async_remote_copy(
            src_ref=o.at[lax.rem(g + 1, 2), tokens(1 - core)], dst_ref=out.at[:, columns(g)], send_sem=osend.at[g], recv_sem=orecv.at[g],
            device_id={"sp": mate}, device_id_type=MESH)

    for c in load(1, 0):
        c.start()
    lent = load(0, 1, r_hbm)

    @pl.when(chip == 0)
    def _():
        for c in lent:
            c.start()

    first_weights = pltpu.make_async_copy(wo.at[:, pl.ds(0, TILE)], w0, wsem)
    first_weights.start()
    barrier = pltpu.get_barrier_semaphore()
    for device in (mate, peer):
        pl.semaphore_signal(barrier, inc=1, device_id={"sp": device}, device_id_type=MESH)
    pl.semaphore_wait(barrier, 2)

    def give(p):
        two = pl.ds(2 * p, 2)
        return pltpu.make_async_remote_copy(
            src_ref=part.at[two], dst_ref=part.at[two], send_sem=psend.at[p], recv_sem=precv.at[p],
            device_id={"sp": peer}, device_id_type=MESH)

    def give_found(p):
        return pltpu.make_async_remote_copy(
            src_ref=found.at[p], dst_ref=other.at[p], send_sem=fsem.at[0, p], recv_sem=fsem.at[1, p],
            device_id={"sp": peer}, device_id_type=MESH)

    def attention(slot, first, heads, lent=None):
        items = [(h, i) for h in heads for i in range(2 * OWN // STRIP)]
        scores, weights = {}, {}

        def end(i):
            return 2 * OWN + (i + 1) * STRIP if lent is None else 4 * OWN

        def strip(i):
            return slice(i * STRIP, (i + 1) * STRIP)

        def score(t):
            h, i = items[t]
            head = slice(h * HEAD, (h + 1) * HEAD) if lent is None else pl.ds(pl.multiple_of((2 * lent + h) * HEAD, HEAD), HEAD)
            queries = q[slot, strip(i), head]
            scores[t] = [dot(k[slot, a : a + STRIP, :], queries, 1, 1) for a in range(first, end(i), STRIP)]

        def weigh(t):
            s = scores.pop(t)
            if lent is None:
                ok = lax.broadcasted_iota(jnp.int32, (STRIP, STRIP), 0) <= lax.broadcasted_iota(jnp.int32, (STRIP, STRIP), 1)
                s = s[:-1] + [jnp.where(ok, s[-1], HIDDEN)]
            top = functools.reduce(jnp.maximum, [x.max(axis=0, keepdims=True) for x in s])
            weights[t] = [jnp.exp2((x - top) * E2).astype(BF) for x in s], top

        def mix(t):
            h, i = items[t]
            p, top = weights.pop(t)
            values = jnp.concatenate([v[slot, :, first : end(i)], jnp.ones((16, end(i) - first), BF)], 0)
            m = dot(values, jnp.concatenate(p, 0))
            total = m[HEAD : HEAD + 1]
            m = m[:HEAD] * (1 / total)
            if lent is not None:
                part[2 * lent + h, :, strip(i)] = m.astype(BF)
                found[lent, h : h + 1, strip(i)] = top * E2 + jnp.log2(total)
                return
            if first:
                here, there = top * E2 + jnp.log2(total), other[h // 2, h % 2 : h % 2 + 1, strip(i)]
                most = jnp.maximum(here, there)
                here, there = jnp.exp2(here - most), jnp.exp2(there - most)
                m = (m * here + part[h, :, strip(i)].astype(F32) * there) * (1 / (here + there))
            o[slot, strip(i), h * HEAD : (h + 1) * HEAD] = m.T.astype(BF)

        for t in range(len(items) + 2):
            if t < len(items):
                score(t)
            if 0 <= t - 1 < len(items):
                weigh(t - 1)
            if 0 <= t - 2 < len(items):
                mix(t - 2)

    @pl.when(chip == 0)
    def _():
        other[...] = jnp.full(other.shape, NEG, F32)
        for c in lent:
            c.wait()

        def two(p, _):
            attention(1, 2 * OWN, range(2), p)
            give_found(p).start()
            give(p).start()

        found[...] = jnp.zeros(found.shape, F32)
        lax.fori_loop(0, GROUP // 2, two, None)

    def group(j, _):
        g, slot = lax.rem(j + 1, 4), lax.rem(j, 2)
        for c in load(g, slot):
            c.wait()

        @pl.when(j < 3)
        def _():
            for c in load(lax.rem(j + 2, 4), 1 - slot):
                c.start()

        @pl.when(j >= 2)
        def _():
            leave(j - 1).wait_send()

        def taken(pairs):
            @pl.when((chip == 1) & (j == 3))
            def _():
                for p in pairs:
                    give(p).wait_recv()
                    give_found(p).wait_recv()

        @pl.when((chip == 0) | (j == 3))
        def _():
            taken((0, 1))
            attention(slot, 2 * OWN, range(4))
            taken((2,))
            attention(slot, 2 * OWN, range(4, GROUP))

        @pl.when((chip == 1) & (j < 3))
        def _():
            attention(slot, 0, range(GROUP))

        leave(g).start()
        out[:, columns(g)] = o[slot, tokens(core)]

    lax.fori_loop(0, 4, group, None)
    for g in (3, 0):
        leave(g).wait_send()
    for g in range(4):
        leave(g).wait_recv()

    @pl.when(chip == 0)
    def _():
        for p in range(GROUP // 2):
            give(p).wait_send()
            give_found(p).wait_send()

    first_weights.wait()


def attend(q, k, v, r, wo):
    hbm = pl.BlockSpec(memory_space=pl.ANY)
    dma = pltpu.SemaphoreType.DMA
    return pl.pallas_call(
        _attend,
        in_specs=[hbm] * 5,
        out_specs=[pl.BlockSpec(memory_space=pltpu.VMEM)] * 2,
        out_shape=[pltpu.VMEM((OWN, D), BF), pltpu.VMEM((D, TILE), BF)],
        scratch_shapes=[
            pltpu.VMEM((2, 2 * OWN, GROUP * HEAD), BF), pltpu.VMEM((2, 4 * OWN, HEAD), BF), pltpu.VMEM((2, HEAD, 4 * OWN), BF),
            pltpu.VMEM((2, 2 * OWN, GROUP * HEAD), BF),
            pltpu.VMEM((GROUP, HEAD, 2 * OWN), BF), pltpu.VMEM((3, 8, 2 * OWN), F32), pltpu.VMEM((3, 8, 2 * OWN), F32),
            dma((2, 2)), dma((2, 2, 4)), dma((4,)), dma((4,)), dma, dma((3,)), dma((3,)), dma((2, 3)),
        ],
        compiler_params=pltpu.CompilerParams(collective_id=1, has_side_effects=True, vmem_limit_bytes=44 * 2**20),
        cost_estimate=pl.CostEstimate(flops=24 * 1024 * 1536 * 512, bytes_accessed=16 * 2**20, transcendentals=24 * 1024 * 1536),
        name="attend",
    )(q, k, v, r, wo)


def _out(x_hbm, o, w0, wo, y_hbm, x, w, y, xsem, wsem, ysem):
    tiles = D // TILE

    def cols(t):
        return pl.ds(pl.multiple_of(t * TILE, TILE), TILE)

    def weight(t):
        slot = lax.rem(t, 3)
        return pltpu.make_async_copy(wo.at[:, cols(t)], w.at[slot], wsem.at[slot])

    def residual(t):
        return pltpu.make_async_copy(x_hbm.at[:, cols(t)], x.at[t], xsem.at[t])

    def leave(t):
        slot = lax.rem(t, 2)
        return pltpu.make_async_copy(y.at[slot], y_hbm.at[:, cols(t)], ysem.at[slot])

    weight(1).start()
    residual(0).start()
    residual(1).start()
    weight(2).start()
    product = dot(o[...], w0[...])
    residual(0).wait()
    y[0] = (x[0].astype(F32) + product).astype(BF)
    leave(0).start()

    def tile(t, _):
        @pl.when(t == 1)
        def _():
            weight(1).wait()

        @pl.when(t < tiles - 1)
        def _():
            weight(t + 1).wait()
            residual(t + 1).start()

        residual(t).wait()

        @pl.when(t >= 2)
        def _():
            leave(t - 2).wait()

        @pl.when(t < tiles - 2)
        def _():
            weight(t + 2).start()

        y[lax.rem(t, 2)] = (x[t].astype(F32) + dot(o[...], w[lax.rem(t, 3)])).astype(BF)
        leave(t).start()

    lax.fori_loop(1, tiles, tile, None)
    leave(tiles - 2).wait()
    leave(tiles - 1).wait()


def output(x, o, w0, wo):
    vmem, hbm = pl.BlockSpec(memory_space=pltpu.VMEM), pl.BlockSpec(memory_space=pl.ANY)
    dma = pltpu.SemaphoreType.DMA
    return pl.pallas_call(
        _out,
        in_specs=[hbm, vmem, vmem, hbm],
        out_specs=hbm,
        out_shape=jax.ShapeDtypeStruct((OWN, D), BF),
        scratch_shapes=[
            pltpu.VMEM((D // TILE, OWN, TILE), BF), pltpu.VMEM((3, D, TILE), BF), pltpu.VMEM((2, OWN, TILE), BF),
            dma((D // TILE,)), dma((3,)), dma((2,)),
        ],
        compiler_params=pltpu.CompilerParams(vmem_limit_bytes=44 * 2**20),
        cost_estimate=pl.CostEstimate(flops=2 * OWN * D * D, bytes_accessed=2 * D * D + 6 * OWN * D, transcendentals=0),
        name="output",
    )(x, o, w0, wo)


def solution(mesh):
    def step(x, gain, wq, wk, wv, wo):
        sp = lax.axis_index("sp")
        mate = sp + 1 - 2 * lax.rem(sp, 2)
        q, k, v, r = project(x, gain, *tables(sp * OWN, mate * OWN), wq, wk, wv)
        o, w0 = (pltpu.with_memory_space_constraint(t, pltpu.VMEM) for t in attend(q, k, v, r, wo))
        return output(x, o, w0, wo)

    tokens, whole = P(("dp", "sp"), None), P(None, None)
    return jax.shard_map(
        step,
        mesh=mesh,
        in_specs=(tokens, P(None), whole, whole, whole, whole),
        out_specs=tokens,
        check_vma=False,
    )
```

```python
import functools

import jax
import jax.numpy as jnp
from jax import lax
from jax.experimental import pallas as pl
from jax.experimental.pallas import tpu as pltpu
from jax.sharding import PartitionSpec as P

HEAD = 128
THETA = 10000
NEG = -1e30
HIDDEN = 2 * NEG
E2 = HEAD**-0.5 * 1.4426950408889634
OWN = 512
RUN = 32
D = 6144
HALF = 3072
KVH = 512
BF, F32 = jnp.bfloat16, jnp.float32


def dot(a, b, ca=1, cb=0):
    return lax.dot_general(a, b, (((ca,), (cb,)), ((), ())), preferred_element_type=F32)


def turn(t, cos, sin):
    return (t * cos + pltpu.roll(t, HEAD // 2, 1) * sin).astype(BF)


def tables(first, second):
    half = HEAD // 2
    row = jnp.arange(2 * OWN // RUN + RUN)[:, None]
    n = OWN // RUN
    place = jnp.where(row < n, first + row * RUN, jnp.where(row < 2 * n, second + (row - n) * RUN, row - 2 * n)).astype(F32)
    angle = place * THETA ** (-(jnp.arange(HEAD) % half).astype(F32) / half)
    return jnp.cos(angle), jnp.sin(angle)


GROUP = 6
CHUNK = 128
TILE = 512
TILES = HALF // TILE
MESH = pl.DeviceIdType.MESH


def _project(x_hbm, g_ref, c_ref, s_ref, wq, wk, wv, q_hbm, k_hbm, v_hbm, r_hbm, xs, w, kv, qs, gain, cos, sin, xsem, xsend, xrecv, wsem, kvsem, ksend, krecv, qsem, rsend, rrecv):
    sp = lax.axis_index("sp")
    core, chip = lax.rem(sp, 2), lax.div(sp, 2)
    mate, peer = sp + 1 - 2 * core, lax.rem(sp + 2, 4)

    def rows(i):
        return pl.ds(i * CHUNK, CHUNK)

    def weight(n):
        if isinstance(n, int) and n < 2:
            src = (wk, wv)[n].at[:, pl.ds(pl.multiple_of(core * KVH, KVH), KVH)]
        else:
            src = wq.at[:, pl.ds(pl.multiple_of(core * HALF + (n - 2) * TILE, TILE), TILE)]
        slot = lax.rem(n, 4)
        return pltpu.make_async_copy(src, w.at[slot], wsem.at[slot])

    mine = [pltpu.make_async_copy(x_hbm.at[rows(i)], xs.at[rows(i)], xsem.at[i]) for i in range(OWN // CHUNK)]
    for c in mine:
        c.start()
    barrier = pltpu.get_barrier_semaphore()
    for other in (mate, peer):
        pl.semaphore_signal(barrier, inc=1, device_id={"sp": other}, device_id_type=MESH)
    pl.semaphore_wait(barrier, 2)
    swaps = [
        pltpu.make_async_remote_copy(
            src_ref=xs.at[rows(i)], dst_ref=xs.at[pl.ds(OWN + i * CHUNK, CHUNK)], send_sem=xsend.at[i], recv_sem=xrecv.at[i],
            device_id={"sp": mate}, device_id_type=MESH)
        for i in range(OWN // CHUNK)
    ]
    gain[...] = g_ref[...].astype(F32).reshape(1, D)
    coarse = 2 * OWN // RUN
    fine_c, fine_s = c_ref[coarse:, :], s_ref[coarse:, :]
    sign = jnp.where(lax.broadcasted_iota(jnp.int32, (1, HEAD), 1) < HEAD // 2, -1.0, 1.0)
    for n in range(coarse):
        c, s = c_ref[n : n + 1, :], s_ref[n : n + 1, :]
        cos[n * RUN : (n + 1) * RUN, :] = c * fine_c - s * fine_s
        sin[n * RUN : (n + 1) * RUN, :] = (s * sign) * fine_c + (c * sign) * fine_s

    def norm(at, n):
        wide = xs[pl.ds(at, n), :].astype(F32)
        scale = lax.rsqrt(jnp.mean(wide * wide, -1, keepdims=True) + 1e-6)
        xs[pl.ds(at, n), :] = (wide * scale * gain[...]).astype(BF)

    def turned_to(dst, t, at):
        n = t.shape[0]
        t = t.astype(BF).astype(F32)
        for h in range(TILE // HEAD):
            one = slice(h * HEAD, (h + 1) * HEAD)
            dst[:, one] = turn(t[:, one], cos[pl.ds(at, n), :], sin[pl.ds(at, n), :])

    def leave(s, p):
        block, n = lax.rem(core + s, 2), 2 * s + p
        out = (k_hbm, v_hbm)[p]
        rest = pl.ds(HEAD, KVH - HEAD)
        rest = (rest, slice(None)) if p else (slice(None), rest)
        return (
            pltpu.make_async_copy(kv.at[n], out.at[2 + block], kvsem.at[n]),
            pltpu.make_async_remote_copy(
                src_ref=kv.at[n, *rest], dst_ref=out.at[block, *rest], send_sem=ksend.at[n], recv_sem=krecv.at[n],
                device_id={"sp": peer}, device_id_type=MESH),
        )

    def send(s, p):
        here, there = leave(s, p)
        here.start()

        @pl.when(chip == 0)
        def _():
            there.start()

    def q_out(tile, s):
        cols = pl.ds(pl.multiple_of(tile * TILE, TILE), TILE)
        part = tile
        return pltpu.make_async_copy(qs.at[part, pl.ds(s * OWN, OWN)], q_hbm.at[lax.rem(core + s, 2), :, cols], qsem.at[part, s])

    def lend(t, s):
        block = lax.rem(core + s, 2)
        cols = pl.ds(t * TILE, TILE if t == 0 else GROUP * HEAD - TILE)
        return pltpu.make_async_remote_copy(
            src_ref=qs.at[t, pl.ds(s * OWN, OWN), pl.ds(0, cols.size)], dst_ref=r_hbm.at[block, :, cols], send_sem=rsend.at[t, s], recv_sem=rrecv.at[t, s],
            device_id={"sp": peer}, device_id_type=MESH)

    def keys(set_):
        turned_to(kv.at[2 * set_], dot(xs[set_ * OWN : (set_ + 1) * OWN, :], w[0]), set_ * OWN)

    def values(set_):
        kv[2 * set_ + 1] = dot(xs[set_ * OWN : (set_ + 1) * OWN, :], w[1]).T.astype(BF)

    for i in range(OWN // CHUNK):
        mine[i].wait()
        if i < 2:
            weight(i).start()
        lax.fori_loop(0, CHUNK // 32, lambda r, _: norm(pl.multiple_of(i * CHUNK + r * 32, 32), 32), None)
        swaps[i].start()
    weight(0).wait()
    keys(0)
    send(0, 0)
    weight(1).wait()
    weight(2).start()
    values(0)
    send(0, 1)
    weight(3).start()
    for c in swaps:
        c.wait_recv()
    weight(2).wait()
    keys(1)
    values(1)
    send(1, 0)
    send(1, 1)
    weight(4).start()
    weight(5).start()

    def tile(t, _):
        @pl.when(t < TILES - 1)
        def _():
            weight(t + 3).wait()

        turned_to(qs.at[t], dot(xs[...], w[lax.rem(t + 2, 4)]), 0)
        for s in range(2):
            q_out(t, s).start()

        @pl.when(t < TILES - 4)
        def _():
            weight(t + 6).start()

        for first in range(2):

            @pl.when((t == first) & (chip == 1))
            def _():
                for s in range(2):
                    lend(first, s).start()

    lax.fori_loop(0, TILES, tile, None)
    for t in range(TILES):
        for s in range(2):
            q_out(t, s).wait()
    for c in swaps:
        c.wait_send()
    for s in range(2):
        for t in range(2):

            @pl.when(chip == 1)
            def _():
                lend(t, s).wait_send()

            @pl.when(chip == 0)
            def _():
                lend(t, s).wait_recv()

        for p in range(2):
            here, there = leave(s, p)
            here.wait()

            @pl.when(chip == 0)
            def _():
                there.wait_send()

            @pl.when(chip == 1)
            def _():
                there.wait_recv()


def project(x, gain, cos, sin, wq, wk, wv):
    vmem, hbm = pl.BlockSpec(memory_space=pltpu.VMEM), pl.BlockSpec(memory_space=pl.ANY)
    dma = pltpu.SemaphoreType.DMA
    return pl.pallas_call(
        _project,
        in_specs=[hbm, vmem, vmem, vmem, hbm, hbm, hbm],
        out_specs=[hbm] * 4,
        out_shape=[
            jax.ShapeDtypeStruct((2, OWN, HALF), BF),
            jax.ShapeDtypeStruct((4, OWN, KVH), BF),
            jax.ShapeDtypeStruct((4, KVH, OWN), BF),
            jax.ShapeDtypeStruct((2, OWN, GROUP * HEAD), BF),
        ],
        scratch_shapes=[
            pltpu.VMEM((2 * OWN, D), BF), pltpu.VMEM((4, D, TILE), BF), pltpu.VMEM((4, OWN, KVH), BF), pltpu.VMEM((TILES, 2 * OWN, TILE), BF),
            pltpu.VMEM((1, D), F32), pltpu.VMEM((2 * OWN, HEAD), F32), pltpu.VMEM((2 * OWN, HEAD), F32),
            dma((4,)), dma((4,)), dma((4,)), dma((4,)), dma((4,)), dma((4,)), dma((4,)), dma((TILES, 2)), dma((2, 2)), dma((2, 2)),
        ],
        compiler_params=pltpu.CompilerParams(collective_id=0, has_side_effects=True, vmem_limit_bytes=62 * 2**20),
        cost_estimate=pl.CostEstimate(flops=4 * OWN * D * (HALF + 2 * KVH), bytes_accessed=2 * D * (HALF + 2 * KVH) + 8 * OWN * D, transcendentals=0),
        name="project",
    )(x, gain, cos, sin, wq, wk, wv)


STRIP = 256


def _attend(q_hbm, k_hbm, v_hbm, r_hbm, wo, out, w0, q, k, v, o, part, found, other, qsem, ksem, osend, orecv, wsem, psend, precv, fsem):
    sp = lax.axis_index("sp")
    core, chip = lax.rem(sp, 2), lax.div(sp, 2)
    mate, peer = sp + 1 - 2 * core, lax.rem(sp + 2, 4)

    def load(g, slot, q_hbm=q_hbm):
        wide, one = pl.ds(pl.multiple_of(g * GROUP * HEAD, HEAD), GROUP * HEAD), pl.ds(pl.multiple_of(g * HEAD, HEAD), HEAD)
        return (
            [pltpu.make_async_copy(q_hbm.at[b, :, wide], q.at[slot, pl.ds(b * OWN, OWN)], qsem.at[slot, b]) for b in range(2)]
            + [pltpu.make_async_copy(k_hbm.at[b, :, one], k.at[slot, pl.ds(b * OWN, OWN)], ksem.at[slot, 0, b]) for b in range(4)]
            + [pltpu.make_async_copy(v_hbm.at[b, one, :], v.at[slot, :, pl.ds(b * OWN, OWN)], ksem.at[slot, 1, b]) for b in range(4)]
        )

    first_heads = 4 * HEAD

    def columns(g, piece=None):
        at, n = {None: (0, GROUP * HEAD), 0: (0, first_heads), 1: (first_heads, GROUP * HEAD - first_heads)}[piece]
        return pl.ds(pl.multiple_of(core * HALF + g * GROUP * HEAD + at, HEAD), n)

    def tokens(c):
        return pl.ds(pl.multiple_of(c * OWN, OWN), OWN)

    def leave(g, piece):
        cols = (pl.ds(0, first_heads), pl.ds(first_heads, GROUP * HEAD - first_heads))[piece]
        return pltpu.make_async_remote_copy(
            src_ref=o.at[lax.rem(g + 1, 2), tokens(1 - core), cols], dst_ref=out.at[:, columns(g, piece)],
            send_sem=osend.at[g, piece], recv_sem=orecv.at[g, piece], device_id={"sp": mate}, device_id_type=MESH)

    for c in load(1, 0):
        c.start()
    lent = load(0, 1, r_hbm)

    @pl.when(chip == 0)
    def _():
        for c in lent:
            c.start()

    first_weights = pltpu.make_async_copy(wo.at[:, pl.ds(0, TILE)], w0, wsem)
    first_weights.start()
    barrier = pltpu.get_barrier_semaphore()
    for device in (mate, peer):
        pl.semaphore_signal(barrier, inc=1, device_id={"sp": device}, device_id_type=MESH)
    pl.semaphore_wait(barrier, 2)

    def give(p):
        two = pl.ds(2 * p, 2)
        return pltpu.make_async_remote_copy(
            src_ref=part.at[two], dst_ref=part.at[two], send_sem=psend.at[p], recv_sem=precv.at[p],
            device_id={"sp": peer}, device_id_type=MESH)

    def give_found(p):
        return pltpu.make_async_remote_copy(
            src_ref=found.at[p], dst_ref=other.at[p], send_sem=fsem.at[0, p], recv_sem=fsem.at[1, p],
            device_id={"sp": peer}, device_id_type=MESH)

    def attention(slot, first, heads, lent=None):
        strips = range(2 * OWN // STRIP)
        items = [(h, i) for h in heads for i in (strips[::-1] if h == heads[-1] else strips)]
        scores, weights = {}, {}

        def end(i):
            return 2 * OWN + (i + 1) * STRIP if lent is None else 4 * OWN

        def strip(i):
            return slice(i * STRIP, (i + 1) * STRIP)

        def score(t):
            h, i = items[t]
            head = slice(h * HEAD, (h + 1) * HEAD) if lent is None else pl.ds(pl.multiple_of((2 * lent + h) * HEAD, HEAD), HEAD)
            queries = q[slot, strip(i), head]
            scores[t] = [dot(k[slot, a : a + STRIP, :], queries, 1, 1) for a in range(first, end(i), STRIP)]

        def weigh(t):
            s = scores.pop(t)
            if lent is None:
                ok = lax.broadcasted_iota(jnp.int32, (STRIP, STRIP), 0) <= lax.broadcasted_iota(jnp.int32, (STRIP, STRIP), 1)
                s = s[:-1] + [jnp.where(ok, s[-1], HIDDEN)]
            top = functools.reduce(jnp.maximum, [x.max(axis=0, keepdims=True) for x in s])
            weights[t] = [jnp.exp2((x - top) * E2).astype(BF) for x in s], top

        def mix(t):
            h, i = items[t]
            p, top = weights.pop(t)
            values = jnp.concatenate([v[slot, :, first : end(i)], jnp.ones((16, end(i) - first), BF)], 0)
            m = dot(values, jnp.concatenate(p, 0))
            total = m[HEAD : HEAD + 1]
            m = m[:HEAD] * (1 / total)
            if lent is not None:
                part[2 * lent + h, :, strip(i)] = m.astype(BF)
                found[lent, h : h + 1, strip(i)] = top * E2 + jnp.log2(total)
                return
            if first:
                here, there = top * E2 + jnp.log2(total), other[h // 2, h % 2 : h % 2 + 1, strip(i)]
                most = jnp.maximum(here, there)
                here, there = jnp.exp2(here - most), jnp.exp2(there - most)
                m = (m * here + part[h, :, strip(i)].astype(F32) * there) * (1 / (here + there))
            o[slot, strip(i), h * HEAD : (h + 1) * HEAD] = m.T.astype(BF)

        for t in range(len(items) + 2):
            if t < len(items):
                score(t)
            if 0 <= t - 1 < len(items):
                weigh(t - 1)
            if 0 <= t - 2 < len(items):
                mix(t - 2)

    @pl.when(chip == 0)
    def _():
        other[...] = jnp.full(other.shape, NEG, F32)
        for c in lent:
            c.wait()

        def two(p, _):
            attention(1, 2 * OWN, range(2), p)
            give_found(p).start()
            give(p).start()

        found[...] = jnp.zeros(found.shape, F32)
        lax.fori_loop(0, GROUP // 2, two, None)

    def group(j, _):
        g, slot = lax.rem(j + 1, 4), lax.rem(j, 2)
        for c in load(g, slot):
            c.wait()

        @pl.when(j < 3)
        def _():
            for c in load(lax.rem(j + 2, 4), 1 - slot):
                c.start()

        @pl.when(j >= 2)
        def _():
            for piece in range(2):
                leave(j - 1, piece).wait_send()

        def taken(pairs):
            @pl.when((chip == 1) & (j == 3))
            def _():
                for p in pairs:
                    give(p).wait_recv()
                    give_found(p).wait_recv()

        @pl.when((chip == 0) | (j == 3))
        def _():
            taken((0, 1))
            attention(slot, 2 * OWN, range(4))
            leave(g, 0).start()
            taken((2,))
            attention(slot, 2 * OWN, range(4, GROUP))

        @pl.when((chip == 1) & (j < 3))
        def _():
            attention(slot, 0, range(GROUP))
            leave(g, 0).start()

        leave(g, 1).start()
        out[:, columns(g)] = o[slot, tokens(core)]

    lax.fori_loop(0, 4, group, None)
    for piece in range(2):
        for g in (3, 0):
            leave(g, piece).wait_send()
        for g in range(4):
            leave(g, piece).wait_recv()

    @pl.when(chip == 0)
    def _():
        for p in range(GROUP // 2):
            give(p).wait_send()
            give_found(p).wait_send()

    first_weights.wait()


def attend(q, k, v, r, wo):
    hbm = pl.BlockSpec(memory_space=pl.ANY)
    dma = pltpu.SemaphoreType.DMA
    return pl.pallas_call(
        _attend,
        in_specs=[hbm] * 5,
        out_specs=[pl.BlockSpec(memory_space=pltpu.VMEM)] * 2,
        out_shape=[pltpu.VMEM((OWN, D), BF), pltpu.VMEM((D, TILE), BF)],
        scratch_shapes=[
            pltpu.VMEM((2, 2 * OWN, GROUP * HEAD), BF), pltpu.VMEM((2, 4 * OWN, HEAD), BF), pltpu.VMEM((2, HEAD, 4 * OWN), BF),
            pltpu.VMEM((2, 2 * OWN, GROUP * HEAD), BF),
            pltpu.VMEM((GROUP, HEAD, 2 * OWN), BF), pltpu.VMEM((3, 8, 2 * OWN), F32), pltpu.VMEM((3, 8, 2 * OWN), F32),
            dma((2, 2)), dma((2, 2, 4)), dma((4, 2)), dma((4, 2)), dma, dma((3,)), dma((3,)), dma((2, 3)),
        ],
        compiler_params=pltpu.CompilerParams(collective_id=1, has_side_effects=True, vmem_limit_bytes=44 * 2**20),
        cost_estimate=pl.CostEstimate(flops=24 * 1024 * 1536 * 512, bytes_accessed=16 * 2**20, transcendentals=24 * 1024 * 1536),
        name="attend",
    )(q, k, v, r, wo)


def _out(x_hbm, o, w0, wo, y_hbm, x, w, y, xsem, wsem, ysem):
    tiles = D // TILE

    def cols(t):
        return pl.ds(pl.multiple_of(t * TILE, TILE), TILE)

    def weight(t):
        slot = lax.rem(t, 3)
        return pltpu.make_async_copy(wo.at[:, cols(t)], w.at[slot], wsem.at[slot])

    def residual(t):
        return pltpu.make_async_copy(x_hbm.at[:, cols(t)], x.at[t], xsem.at[t])

    def leave(t):
        slot = lax.rem(t, 2)
        return pltpu.make_async_copy(y.at[slot], y_hbm.at[:, cols(t)], ysem.at[slot])

    weight(1).start()
    residual(0).start()
    residual(1).start()
    weight(2).start()
    product = dot(o[...], w0[...])
    residual(0).wait()
    y[0] = (x[0].astype(F32) + product).astype(BF)
    leave(0).start()

    def tile(t, _):
        @pl.when(t == 1)
        def _():
            weight(1).wait()

        @pl.when(t < tiles - 1)
        def _():
            weight(t + 1).wait()
            residual(t + 1).start()

        residual(t).wait()

        @pl.when(t >= 2)
        def _():
            leave(t - 2).wait()

        @pl.when(t < tiles - 2)
        def _():
            weight(t + 2).start()

        y[lax.rem(t, 2)] = (x[t].astype(F32) + dot(o[...], w[lax.rem(t, 3)])).astype(BF)
        leave(t).start()

    lax.fori_loop(1, tiles, tile, None)
    leave(tiles - 2).wait()
    leave(tiles - 1).wait()


def output(x, o, w0, wo):
    vmem, hbm = pl.BlockSpec(memory_space=pltpu.VMEM), pl.BlockSpec(memory_space=pl.ANY)
    dma = pltpu.SemaphoreType.DMA
    return pl.pallas_call(
        _out,
        in_specs=[hbm, vmem, vmem, hbm],
        out_specs=hbm,
        out_shape=jax.ShapeDtypeStruct((OWN, D), BF),
        scratch_shapes=[
            pltpu.VMEM((D // TILE, OWN, TILE), BF), pltpu.VMEM((3, D, TILE), BF), pltpu.VMEM((2, OWN, TILE), BF),
            dma((D // TILE,)), dma((3,)), dma((2,)),
        ],
        compiler_params=pltpu.CompilerParams(vmem_limit_bytes=44 * 2**20),
        cost_estimate=pl.CostEstimate(flops=2 * OWN * D * D, bytes_accessed=2 * D * D + 6 * OWN * D, transcendentals=0),
        name="output",
    )(x, o, w0, wo)


def solution(mesh):
    def step(x, gain, wq, wk, wv, wo):
        sp = lax.axis_index("sp")
        mate = sp + 1 - 2 * lax.rem(sp, 2)
        q, k, v, r = project(x, gain, *tables(sp * OWN, mate * OWN), wq, wk, wv)
        o, w0 = (pltpu.with_memory_space_constraint(t, pltpu.VMEM) for t in attend(q, k, v, r, wo))
        return output(x, o, w0, wo)

    tokens, whole = P(("dp", "sp"), None), P(None, None)
    return jax.shard_map(
        step,
        mesh=mesh,
        in_specs=(tokens, P(None), whole, whole, whole, whole),
        out_specs=tokens,
        check_vma=False,
    )
```
